8 devices in a mesh: rep: 1 (over z), dp: 8 (over x, y, core).
Axes of the slice: x: 2, y: 2, z: 1, core: 2. Of those that a mesh axis runs over, the one named last changes fastest.
Arguments:
- x: bfloat16 [8, 2048, 1024], P(('rep', 'dp'))
- dy: bfloat16 [8, 2048, 1024], P(('rep', 'dp'))
- w_gate: bfloat16 [2, 1024, 2816], replicated
- w_up: bfloat16 [2, 1024, 2816], replicated
- w_down: bfloat16 [2, 2816, 1024], replicated
- m_w_gate: float32 [2, 1024, 2816], P(None, 'dp')
- m_w_up: float32 [2, 1024, 2816], P(None, 'dp')
- m_w_down: float32 [2, 2816, 1024], P(None, 'dp')
- v_w_gate: float32 [2, 1024, 2816], P(None, 'dp')
- v_w_up: float32 [2, 1024, 2816], P(None, 'dp')
- v_w_down: float32 [2, 2816, 1024], P(None, 'dp')
Outputs:
- output 1: bfloat16 [2, 1024, 2816], P('rep')
- output 2: bfloat16 [2, 1024, 2816], P('rep')
- output 3: bfloat16 [2, 2816, 1024], P('rep')
- output 4: float32 [2, 1024, 2816], P('rep', 'dp')
- output 5: float32 [2, 1024, 2816], P('rep', 'dp')
- output 6: float32 [2, 2816, 1024], P('rep', 'dp')
- output 7: float32 [2, 1024, 2816], P('rep', 'dp')
- output 8: float32 [2, 1024, 2816], P('rep', 'dp')
- output 9: float32 [2, 2816, 1024], P('rep', 'dp')
All inputs are finite; a program needn't handle non-finite values.
Results may differ from the reference program's by a relative error of at most 0.022.
Values are sent between devices in bfloat16 or wider.
A program may use at most 2 GiB of HBM per device.

```python
import jax
import jax.numpy as jnp
from jax import lax

SEQUENCES = 8
TOKENS = 2048
D = 1024
FF = 2816
LAYERS = 2
NAMES = ("w_gate", "w_up", "w_down")
SHAPES = {"w_gate": (LAYERS, D, FF), "w_up": (LAYERS, D, FF), "w_down": (LAYERS, FF, D)}


def bump(key, n, height):
    away = (jnp.arange(n, dtype=jnp.int32) - jax.random.randint(key, (), 0, n, jnp.int32)) % n
    return jnp.where(away < n // 8, height, 1.0)


def together(key, own, strength):
    shared = jax.random.normal(key, own.shape[1:], jnp.float32)
    return (own + strength * shared) * lax.rsqrt(1 + strength * strength)


def setup_inputs(seed: int = 0, part: int = 0) -> dict:
    kx, kdy, ka, kb, kz, kf, kh, kl, *keys = jax.random.split(jax.random.key(seed), 8 + 3 * len(NAMES))
    kx, kdy, ka, kb = (jax.random.fold_in(k, part) for k in (kx, kdy, ka, kb))
    kw, km, kv = (keys[i::3] for i in range(3))
    shape = (SEQUENCES, TOKENS, D)
    much_x, much_dy = jax.random.uniform(kz, (2,), jnp.float32, 0.0, 1.0)
    loud = 2.0 ** jax.random.uniform(jax.random.fold_in(kz, 1), (), jnp.float32, -1.0, 2.0)
    layers = 2.0 ** jax.random.uniform(kl, (LAYERS, 1, 1), jnp.float32, -1.0, 1.0)
    x = together(ka, jax.random.normal(kx, shape, jnp.float32), much_x) * bump(kf, D, 4.0)
    dy = together(kb, jax.random.normal(kdy, shape, jnp.float32), much_dy)
    drawn = {"x": x.astype(jnp.bfloat16), "dy": (loud * dy * (SEQUENCES * TOKENS) ** -0.5).astype(jnp.bfloat16)}
    for key, name in zip(kw, NAMES, strict=True):
        w = jax.random.normal(key, SHAPES[name], jnp.float32) * SHAPES[name][1] ** -0.5
        drawn[name] = (w * {"w_gate": 1.0, "w_up": bump(kh, FF, 4.0), "w_down": layers}[name]).astype(jnp.bfloat16)
    for key, name in zip(km, NAMES, strict=True):
        drawn[f"m_{name}"] = 0.1 * jax.random.normal(key, SHAPES[name], jnp.float32)
    for key, name in zip(kv, NAMES, strict=True):
        drawn[f"v_{name}"] = jax.random.uniform(key, SHAPES[name], jnp.float32, 0.005, 0.015)
    return drawn


def matmul(a, w):
    return jnp.dot(a, w, preferred_element_type=jnp.float32).astype(jnp.bfloat16)


def normed(h):
    wide = h.astype(jnp.float32)
    scale = lax.rsqrt(jnp.mean(wide**2, -1, keepdims=True) + 1e-6)
    return (wide * scale).astype(jnp.bfloat16)


def layer(h, w):
    a = normed(h)
    gate = jnp.dot(a, w["w_gate"], preferred_element_type=jnp.float32)
    up = jnp.dot(a, w["w_up"], preferred_element_type=jnp.float32)
    return h + matmul((jax.nn.silu(gate) * up).astype(jnp.bfloat16), w["w_down"])


def adamw(w, m, v, g):
    m = 0.9 * m + 0.1 * g
    v = 0.95 * v + 0.05 * g * g
    step = m * lax.rsqrt(v + 1e-8) + 0.1 * w
    return (w - 0.02 * step).astype(jnp.bfloat16), m, v


def clipped(gradients, sum_of_squares, count):
    factor = jnp.minimum(1.0, 0.5 * lax.rsqrt(sum_of_squares / count + 1e-30))
    return [g * factor for g in gradients]


def stack(weights, h):
    return lax.scan(lambda h, w: (layer(h, w), None), h, weights)[0]


def reference(x, dy, w_gate, w_up, w_down, m_w_gate, m_w_up, m_w_down, v_w_gate, v_w_up, v_w_down):
    weights = dict(zip(NAMES, (w_gate, w_up, w_down), strict=True))

    def take(so_far, sequence):
        h, by_y = sequence
        _, back = jax.vjp(lambda w: stack(w, h), weights)
        return jax.tree.map(lambda total, term: total + term.astype(jnp.float32), so_far, back(by_y)[0]), None

    none_yet = {name: jnp.zeros(w.shape, jnp.float32) for name, w in weights.items()}
    by_weights, _ = lax.scan(take, none_yet, (x, dy))
    gradients = [by_weights[name].astype(jnp.bfloat16).astype(jnp.float32) for name in NAMES]
    gradients = clipped(gradients, sum(jnp.sum(g * g) for g in gradients), sum(g.size for g in gradients))
    new = [
        adamw(w.astype(jnp.float32), m, v, g)
        for w, m, v, g in zip((w_gate, w_up, w_down), (m_w_gate, m_w_up, m_w_down), (v_w_gate, v_w_up, v_w_down), gradients, strict=True)
    ]
    return tuple(one[which] for which in range(3) for one in new)
```

```python
import functools
import jax
import jax.numpy as jnp
from jax import lax
from jax.experimental import pallas as pl
from jax.experimental.pallas import tpu as pltpu

BF, F32 = jnp.bfloat16, jnp.float32
NB = 256
VM = 64 * 1024 * 1024 - 65536


def dot(a, b, ca=1, cb=0):
    return lax.dot_general(a, b, (((ca,), (cb,)), ((), ())), preferred_element_type=F32)


def normed(h):
    wide = h.astype(F32)
    scale = lax.rsqrt(jnp.mean(wide * wide, -1, keepdims=True) + 1e-6)
    return (wide * scale).astype(BF)


def params():
    return pltpu.CompilerParams(vmem_limit_bytes=VM, dimension_semantics=("arbitrary",))


def whole(shape):
    return pl.BlockSpec(shape, lambda j: (0,) * len(shape))


def cost(mm, by):
    return pl.CostEstimate(flops=mm, bytes_accessed=by, transcendentals=0)


def tiles(t, rt):
    return [pl.ds(i * rt, rt) for i in range(t // rt)]


def fwd0(x, wg, wu, wd, layer, rt=512):
    t, d = x.shape
    ff = wg.shape[2]

    def body(x_ref, wg_ref, wu_ref, wd_ref, gate_ref, up_ref, a_ref, h_ref, b_ref, acc):
        j = pl.program_id(0)

        @pl.when(j == 0)
        def _():
            for r in tiles(t, 256):
                a_ref[r, :] = normed(x_ref[r, :])
                acc[r, :] = jnp.zeros((256, d), F32)

        for r in tiles(t, rt):
            a = a_ref[r, :]
            gate = dot(a, wg_ref[...])
            up = dot(a, wu_ref[...])
            gate_ref[r, :] = gate
            up_ref[r, :] = up
            acc[r, :] += dot((jax.nn.silu(gate) * up).astype(BF), wd_ref[...])

        @pl.when(j == pl.num_programs(0) - 1)
        def _():
            for r in tiles(t, 256):
                h = x_ref[r, :] + acc[r, :].astype(BF)
                h_ref[r, :] = h
                b_ref[r, :] = normed(h)

    one = pl.Buffered(1)
    return pl.pallas_call(
        body,
        grid=(ff // NB,),
        in_specs=[
            whole((t, d)),
            pl.BlockSpec((None, d, NB), lambda j: (layer, 0, j)),
            pl.BlockSpec((None, d, NB), lambda j: (layer, 0, j)),
            pl.BlockSpec((None, NB, d), lambda j: (layer, j, 0)),
        ],
        out_specs=[
            pl.BlockSpec((t, NB), lambda j: (0, j)),
            pl.BlockSpec((t, NB), lambda j: (0, j)),
            whole((t, d)),
            whole((t, d)),
            whole((t, d)),
        ],
        out_shape=[jax.ShapeDtypeStruct((t, ff), F32)] * 2 + [jax.ShapeDtypeStruct((t, d), BF)] * 3,
        scratch_shapes=[pltpu.VMEM((t, d), F32)],
        compiler_params=params(),
        cost_estimate=cost(6 * t * d * ff, 0),
        name="fwd0",
    )(x, wg, wu, wd)


def hidden_back(dh, gate, up):
    s = jax.nn.sigmoid(gate)
    sg = gate * s
    return (dh * up * (s + sg * (1 - s))).astype(BF), (dh * sg).astype(BF), sg


S = 4
MESH = pl.DeviceIdType.MESH
GU, DD = 256, 352


class Exchange:
    def __init__(self, src, rc, sx, sy, rx, ry, s2, r2, sent, got, squares, put):
        self.src, self.rc, self.sx, self.sy, self.rx, self.ry, self.s2, self.r2 = src, rc, sx, sy, rx, ry, s2, r2
        self.sent, self.got, self.squares, self.put = sent, got, squares, put
        me = lax.axis_index("dp")
        self.x, self.y, self.c = me // 4, me // 2 % 2, me % 2
        self.over_c, self.over_y, self.over_x = me + 1 - 2 * self.c, me + 2 - 4 * self.y, me + 4 - 8 * self.x

    def barrier(self):
        b = pltpu.get_barrier_semaphore()
        for other in (self.over_c, self.over_y, self.over_x):
            pl.semaphore_signal(b, inc=1, device_id={"dp": other}, device_id_type=MESH)
        pl.semaphore_wait(b, 3)

    def copy(self, n, slot, src, dst, other):
        return pltpu.make_async_remote_copy(
            src_ref=src, dst_ref=dst, send_sem=self.sent.at[n, slot], recv_sem=self.got.at[n, slot],
            device_id={"dp": other}, device_id_type=MESH,
        )

    def copies(self, stage, k, rows):
        s, h = lax.rem(k, S), rows // 2
        if stage == 0:
            return [self.copy(0, s, self.src.at[s, :, 1 - self.c, :rows], self.rc.at[s, :, :rows], self.over_c)]
        if stage == 1:
            return [
                self.copy(1, s, self.sx.at[s, :, :h], self.rx.at[s, :, :h], self.over_x),
                self.copy(2, s, self.sy.at[s, :, :h], self.ry.at[s, :, :h], self.over_y),
            ]
        return [
            self.copy(3, s, self.s2.at[s, 0, :h], self.r2.at[s, 0, :h], self.over_y),
            self.copy(4, s, self.s2.at[s, 1, :h], self.r2.at[s, 1, :h], self.over_x),
        ]

    def start(self, stage, k, rows):
        for c in self.copies(stage, k, rows):
            c.start()

    def chip(self, s, i, j, part):
        at = i * 2 + j
        return self.src[s, at, self.c, part, :].astype(F32) + self.rc[s, at, part, :].astype(F32)

    def stage(self, n, k, rows):
        for c in self.copies(n - 1, k, rows):
            c.wait()
        s, h, x, y = lax.rem(k, S), rows // 2, self.x, self.y
        a, b = slice(0, h), slice(h, rows)
        if n == 1:
            for i in range(2):
                self.sx[s, i, a, :] = self.chip(s, 1 - x, i, a).astype(BF)
                self.sy[s, i, a, :] = self.chip(s, i, 1 - y, b).astype(BF)
        elif n == 2:
            self.s2[s, 0, a, :] = (self.chip(s, x, 1 - y, a) + self.rx[s, 1 - y, a, :].astype(F32)).astype(BF)
            self.s2[s, 1, a, :] = (self.chip(s, 1 - x, y, b) + self.ry[s, 1 - x, a, :].astype(F32)).astype(BF)
        else:
            first = self.chip(s, x, y, a) + self.rx[s, y, a, :].astype(F32) + self.r2[s, 0, a, :].astype(F32)
            second = self.chip(s, x, y, b) + self.ry[s, x, a, :].astype(F32) + self.r2[s, 1, a, :].astype(F32)
            first, second = first.astype(BF), second.astype(BF)
            self.put(k, rows, first, second)
            for g in (first, second):
                g = g.astype(F32)
                self.squares[...] += jnp.sum(g * g, 0, keepdims=True)
        if n < 3:
            self.start(n, k, rows)

    def tick(self, t, gu, dd):
        for n, k in ((3, t - 4), (2, t - 3), (1, t - 2), (0, t - 1)):
            for low, high, rows in ((0, gu, GU), (gu, gu + dd, DD)):

                @pl.when((k >= low) & (k < high))
                def _():
                    if n:
                        self.stage(n, k, rows)
                    else:
                        self.start(0, k, rows)


def exchange_scratch():
    return [
        pltpu.VMEM((S, 4, 2, DD, NB), BF),
        pltpu.VMEM((S, 4, DD, NB), BF),
    ] + [pltpu.VMEM((S, 2, DD // 2, NB), BF)] * 6 + [pltpu.SemaphoreType.DMA((5, S))] * 2


def backward(a, dh, h, gate, up, wg, wu, wd, layer, collective_id):
    t_, d = a.shape
    ff = wg.shape[2]
    n_gu, n_dd = ff // NB, d // NB
    last = n_gu + n_dd + 3
    inner = h is not None

    def body(*refs):
        if inner:
            a_hbm, dh_ref, h_hbm, wg_ref, wu_ref, wd_ref, rg_ref, ru_ref, rd_ref, sq_ref, o_hbm, abuf, acc, io, *refs = refs
        else:
            a_hbm, dh_ref, gate_ref, up_ref, wd_ref, rg_ref, ru_ref, rd_ref, sq_ref, abuf, io, *refs = refs
        at, ht, dg, du, *refs = refs
        t = pl.program_id(0)

        def put(k, rows, first, second):
            if rows == GU:
                cols = pl.ds(pl.multiple_of(k * NB, NB), NB)
                rg_ref[:, cols] = first
                ru_ref[:, cols] = second
            else:
                cols = pl.ds(pl.multiple_of((k - n_gu) * NB, NB), NB)
                rd_ref[: DD // 2, cols] = first
                rd_ref[DD // 2 :, cols] = second

        ex = Exchange(*refs, sq_ref, put)

        @pl.when(t == 0)
        def _():
            ex.barrier()
            sq_ref[...] = jnp.zeros_like(sq_ref)
            load = pltpu.make_async_copy(a_hbm, abuf, io)
            load.start()
            if inner:
                for r in tiles(t_, 256):
                    acc[r, :] = jnp.zeros((256, d), F32)
            load.wait()
            for r in tiles(t_, 256):
                at[:, r] = abuf[r, :].T

        ex.tick(t, n_gu, n_dd)
        slot = lax.rem(t, S)

        @pl.when(t < n_gu)
        def _():
            rows = pl.ds(pl.multiple_of(t * NB, NB), NB)
            for r in tiles(t_, 512):
                if inner:
                    gt = dot(abuf[r, :], wg_ref[...])
                    u = dot(abuf[r, :], wu_ref[...])
                else:
                    gt, u = gate_ref[r, :], up_ref[r, :]
                dp = dot(dh_ref[r, :], wd_ref[...], 1, 1).astype(BF).astype(F32)
                dgt, dut, sg = hidden_back(dp, gt, u)
                dg[r, :] = dgt
                du[r, :] = dut
                ht[rows, r] = (sg * u).astype(BF).T
                if inner:
                    acc[r, :] += dot(dgt, wg_ref[...], 1, 1) + dot(dut, wu_ref[...], 1, 1)
            for i in range(2):
                r = pl.ds(i * d // 2, d // 2)
                src = refs[0]
                src[slot, 2 * i : 2 * i + 2, :, : GU // 2, :] = dot(at[r, :], dg[...]).astype(BF).reshape(2, 2, GU // 2, NB)
                src[slot, 2 * i : 2 * i + 2, :, GU // 2 : GU, :] = dot(at[r, :], du[...]).astype(BF).reshape(2, 2, GU // 2, NB)

        @pl.when((t >= n_gu) & (t < n_gu + n_dd))
        def _():
            cols = pl.ds(pl.multiple_of((t - n_gu) * NB, NB), NB)
            for i in range(4):
                r = pl.ds(i * 2 * DD, 2 * DD)
                refs[0][slot, i] = dot(ht[r, :], dh_ref[:, cols]).astype(BF).reshape(2, DD, NB)

        if inner:

            @pl.when(t == n_gu)
            def _():
                pltpu.make_async_copy(h_hbm, abuf, io).start()

            @pl.when(t == n_gu + n_dd)
            def _():
                pltpu.make_async_copy(h_hbm, abuf, io).wait()
                for r in tiles(t_, 256):
                    da = acc[r, :].astype(BF).astype(F32)
                    wide = abuf[r, :].astype(F32)
                    scale = lax.rsqrt(jnp.mean(wide * wide, -1, keepdims=True) + 1e-6)
                    along = jnp.sum(da * wide, -1, keepdims=True) * (scale * scale * scale / d)
                    abuf[r, :] = dh_ref[r, :] + (da * scale - wide * along).astype(BF)

            @pl.when(t == n_gu + n_dd + 1)
            def _():
                pltpu.make_async_copy(abuf, o_hbm, io).start()

            @pl.when(t == last)
            def _():
                pltpu.make_async_copy(abuf, o_hbm, io).wait()

    def block(j):
        return jnp.minimum(j, n_gu - 1)

    once = pl.Buffered(1)
    anyw = pl.BlockSpec(memory_space=pl.ANY)
    dh_spec = pl.BlockSpec((t_, d), lambda j: (0, 0), pipeline_mode=once)
    wcol = pl.BlockSpec((None, d, NB), lambda j: (layer, 0, block(j)))
    wrow = pl.BlockSpec((None, NB, d), lambda j: (layer, block(j), 0))
    gcol = pl.BlockSpec((t_, NB), lambda j: (0, block(j)))
    in_specs = [anyw, dh_spec, anyw, wcol, wcol, wrow] if inner else [anyw, dh_spec, gcol, gcol, wrow]
    args = (a, dh, h, wg, wu, wd) if inner else (a, dh, gate, up, wd)
    shapes = [(d // 8, ff), (d // 8, ff), (ff // 8, d)]
    out_specs = [whole(s) for s in shapes] + [whole((1, NB))] + ([anyw] if inner else [])
    out_shape = [jax.ShapeDtypeStruct(s, BF) for s in shapes] + [jax.ShapeDtypeStruct((1, NB), F32)]
    out_shape += [jax.ShapeDtypeStruct((t_, d), BF)] if inner else []
    scratch = [pltpu.VMEM((t_, d), BF)] + ([pltpu.VMEM((t_, d), F32)] if inner else []) + [pltpu.SemaphoreType.DMA]
    scratch += [pltpu.VMEM((d, t_), BF), pltpu.VMEM((ff, t_), BF)] + [pltpu.VMEM((t_, NB), BF)] * 2
    return pl.pallas_call(
        body,
        grid=(last + 1,),
        in_specs=in_specs,
        out_specs=out_specs,
        out_shape=out_shape,
        scratch_shapes=scratch + exchange_scratch(),
        compiler_params=pltpu.CompilerParams(
            vmem_limit_bytes=VM, dimension_semantics=("arbitrary",), collective_id=collective_id, has_side_effects=True
        ),
        cost_estimate=cost((16 if inner else 8) * t_ * d * ff, 0),
        name=f"backward{layer}",
    )(*args)


def swap(bit):
    return [(i, i ^ bit) for i in range(8)]


def send(t, bit):
    return lax.ppermute(t, "dp", swap(bit))


def pick(t, i, axis):
    return lax.dynamic_index_in_dim(t, i, axis, keepdims=False)


def gather(own, x, y, c):
    layers, rows, n = own.shape
    from_x, from_y = send(own, 4), send(own, 2)
    corner0, corner1 = send(from_x[0], 2), send(from_y[1], 4)
    pieces = []
    for t, fx, fy in ((own, 0, 0), (from_x, 1, 0), (from_y, 0, 1)):
        pieces.append((t, x ^ fx, y ^ fy, c, 0))
        pieces.append((send(t, 1), x ^ fx, y ^ fy, 1 - c, 0))
    for l, t in enumerate((corner0, corner1)):
        pieces.append((t[None], 1 - x, 1 - y, c, l))
        pieces.append((send(t, 1)[None], 1 - x, 1 - y, 1 - c, l))
    out = jnp.zeros((layers, 8 * rows, n), BF)
    for t, i, j, k, l in pieces:
        out = lax.dynamic_update_slice(out, t, (l, ((i * 2 + j) * 2 + k) * rows, 0))
    return out


def adamw(w, m, v, g):
    m = 0.9 * m + 0.1 * g
    v = 0.95 * v + 0.05 * g * g
    step = m * lax.rsqrt(v + 1e-8) + 0.1 * w
    return (w - 0.02 * step).astype(BF), m, v


def solution(mesh):
    def step(x, dy, wg, wu, wd, *moments):
        me = lax.axis_index("dp")
        ix, iy, ic = me // 4, me // 2 % 2, me % 2
        x, dy = x[0], dy[0]

        gate, up, a0, h1, a1 = fwd0(x, wg, wu, wd, 0)
        r_g1, r_u1, r_d1, sq1, dh = backward(a1, dy, h1, None, None, wg, wu, wd, 1, 1)
        r_g0, r_u0, r_d0, sq0 = backward(a0, dh, None, gate, up, wg, wu, wd, 0, 2)
        gs = [jnp.stack(p) for p in ((r_g0, r_g1), (r_u0, r_u1), (r_d0, r_d1))]
        count = sum(w.size for w in (wg, wu, wd))
        total = jnp.sum(sq0 + sq1)
        total = jnp.full((8, 128), total)
        for bit in (1, 2, 4):
            total = total + send(total, bit)
        factor = jnp.minimum(1.0, 0.5 * lax.rsqrt(total[0, 0] / count + 1e-30))
        new = []
        for w, m, v, g in zip((wg, wu, wd), moments[:3], moments[3:], gs):
            rows = m.shape[1]
            own = lax.dynamic_slice_in_dim(w, me * rows, rows, 1)
            own, m, v = adamw(own.astype(F32), m, v, g.astype(F32) * factor)
            new.append((gather(own, ix, iy, ic), m, v))
        return tuple(one[which] for which in range(3) for one in new)

    P = jax.sharding.PartitionSpec
    rows = P(None, "dp", None)
    return jax.shard_map(
        step,
        mesh=mesh,
        in_specs=(P(("rep", "dp")),) * 2 + (P(),) * 3 + (rows,) * 6,
        out_specs=(P("rep"),) * 3 + (P("rep", "dp", None),) * 6,
        check_vma=False,
    )
```

```python
import jax
import jax.numpy as jnp
from jax import lax
from jax.experimental import pallas as pl
from jax.experimental.pallas import tpu as pltpu


BF, F32 = jnp.bfloat16, jnp.float32
NB = 256
VM = 64 * 1024 * 1024 - 65536


def dot(a, b, ca=1, cb=0):
    return lax.dot_general(a, b, (((ca,), (cb,)), ((), ())), preferred_element_type=F32)


def normed(h):
    wide = h.astype(F32)
    scale = lax.rsqrt(jnp.mean(wide * wide, -1, keepdims=True) + 1e-6)
    return (wide * scale).astype(BF)


def params():
    return pltpu.CompilerParams(vmem_limit_bytes=VM, dimension_semantics=("arbitrary",))


def whole(shape):
    return pl.BlockSpec(shape, lambda j: (0,) * len(shape))


def cost(mm, by):
    return pl.CostEstimate(flops=mm, bytes_accessed=by, transcendentals=0)


def tiles(t, rt):
    return [pl.ds(i * rt, rt) for i in range(t // rt)]


def beside(ref, one, other):
    n = one.shape[1]
    ref[:, :n] = one[...]
    ref[:, n:] = other[...]


def fwd0(x, wg, wu, wd, layer):
    t_, d = x.shape
    ff = wg.shape[2]
    n1, rt = ff // NB, 512
    n2 = t_ // rt

    def body(x_hbm, wg_ref, wu_ref, wd_hbm, gate_ref, up_ref, a_hbm, h_ref, b_ref, xs, a, hid, w, wds, sem, wd_sem, a_sem):
        t = pl.program_id(0)
        wd_load = pltpu.make_async_copy(wd_hbm.at[layer], wds, wd_sem)
        a_store = pltpu.make_async_copy(a, a_hbm, a_sem)

        @pl.when(t == 0)
        def _():
            loads = [pltpu.make_async_copy(x_hbm.at[r], xs.at[r], sem.at[i]) for i, r in enumerate(tiles(t_, rt))]
            for load in loads:
                load.start()
            wd_load.start()
            for i, load in enumerate(loads):
                load.wait()
                for r in range(i * rt, (i + 1) * rt, 256):
                    a[pl.ds(r, 256), :] = normed(xs[pl.ds(r, 256), :])

        @pl.when(t == 1)
        def _():
            a_store.start()

        @pl.when(t < n1)
        def _():
            beside(w, wg_ref, wu_ref)
            cols = pl.ds(pl.multiple_of(t * NB, NB), NB)
            for r in tiles(t_, rt):
                both = dot(a[r, :], w[...])
                gate, up = both[:, :NB], both[:, NB:]
                gate_ref[r, :] = gate
                up_ref[r, :] = up
                hid[r, cols] = (jax.nn.silu(gate) * up).astype(BF)

        @pl.when(t == n1)
        def _():
            wd_load.wait()
            a_store.wait()

        @pl.when(t >= n1)
        def _():
            r = pl.ds(pl.multiple_of((t - n1) * rt, rt), rt)
            h = xs[r, :] + dot(hid[r, :], wds[...]).astype(BF)
            h_ref[...] = h
            b_ref[...] = normed(h)

    def block(j):
        return jnp.minimum(j, n1 - 1)

    anyw = pl.BlockSpec(memory_space=pl.ANY)
    wcol = pl.BlockSpec((None, d, NB), lambda j: (layer, 0, block(j)))
    gcol = pl.BlockSpec((t_, NB), lambda j: (0, block(j)))
    hrow = pl.BlockSpec((rt, d), lambda j: (jnp.maximum(j - n1, 0), 0))
    return pl.pallas_call(
        body,
        grid=(n1 + n2,),
        in_specs=[anyw, wcol, wcol, anyw],
        out_specs=[gcol, gcol, anyw, hrow, hrow],
        out_shape=[jax.ShapeDtypeStruct((t_, ff), F32)] * 2 + [jax.ShapeDtypeStruct((t_, d), BF)] * 3,
        scratch_shapes=[
            pltpu.VMEM((t_, d), BF),
            pltpu.VMEM((t_, d), BF),
            pltpu.VMEM((t_, ff), BF),
            pltpu.VMEM((d, 2 * NB), BF),
            pltpu.VMEM((ff, d), BF),
            pltpu.SemaphoreType.DMA((n2,)),
            pltpu.SemaphoreType.DMA,
            pltpu.SemaphoreType.DMA,
        ],
        compiler_params=params(),
        cost_estimate=cost(6 * t_ * d * ff, 0),
        name="forward0",
    )(x, wg, wu, wd)


def hidden_back(dh, gate, up):
    s = jax.nn.sigmoid(gate)
    sg = gate * s
    return (dh * up * (s + sg * (1 - s))).astype(BF), (dh * sg).astype(BF), sg


SRC, RC, SX, RX, S2, R2 = 4, 5, 2, 6, 2, 4
MESH = pl.DeviceIdType.MESH
GU, DD = 256, 352


class Exchange:
    def __init__(self, src, rc, sx, sy, rx, ry, s2, r2, sent, got, squares, put):
        self.src, self.rc, self.sx, self.sy, self.rx, self.ry, self.s2, self.r2 = src, rc, sx, sy, rx, ry, s2, r2
        self.sent, self.got, self.squares, self.put = sent, got, squares, put
        me = lax.axis_index("dp")
        self.x, self.y, self.c = me // 4, me // 2 % 2, me % 2
        self.over_c, self.over_y, self.over_x = me + 1 - 2 * self.c, me + 2 - 4 * self.y, me + 4 - 8 * self.x

    def barrier(self):
        b = pltpu.get_barrier_semaphore()
        for other in (self.over_c, self.over_y, self.over_x):
            pl.semaphore_signal(b, inc=1, device_id={"dp": other}, device_id_type=MESH)
        pl.semaphore_wait(b, 3)

    def copy(self, n, slot, src, dst, other):
        return pltpu.make_async_remote_copy(
            src_ref=src, dst_ref=dst, send_sem=self.sent.at[n, slot], recv_sem=self.got.at[n, slot],
            device_id={"dp": other}, device_id_type=MESH,
        )

    def copies(self, stage, k, rows):
        h = rows // 2
        if stage == 0:
            s, r = lax.rem(k, SRC), lax.rem(k, RC)
            return [self.copy(0, r, self.src.at[s, :, 1 - self.c, :rows], self.rc.at[r, :, :rows], self.over_c)]
        if stage == 1:
            s, r = lax.rem(k, SX), lax.rem(k, RX)
            return [
                self.copy(1, r, self.sx.at[s, :, :h], self.rx.at[r, :, :h], self.over_x),
                self.copy(2, r, self.sy.at[s, :, :h], self.ry.at[r, :, :h], self.over_y),
            ]
        s, r = lax.rem(k, S2), lax.rem(k, R2)
        return [
            self.copy(3, r, self.s2.at[s, 0, :h], self.r2.at[r, 0, :h], self.over_y),
            self.copy(4, r, self.s2.at[s, 1, :h], self.r2.at[r, 1, :h], self.over_x),
        ]

    def start(self, stage, k, rows):
        for c in self.copies(stage, k, rows):
            c.start()

    def chip(self, k, i, j, part):
        at = i * 2 + j
        return self.src[lax.rem(k, SRC), at, self.c, part, :].astype(F32) + self.rc[lax.rem(k, RC), at, part, :].astype(F32)

    def stage(self, n, k, rows):
        for c in self.copies(n - 1, k, rows):
            c.wait()
        h, x, y = rows // 2, self.x, self.y
        a, b = slice(0, h), slice(h, rows)
        sx, rx, s2, r2 = (lax.rem(k, m) for m in (SX, RX, S2, R2))
        if n == 1:
            for i in range(2):
                self.sx[sx, i, a, :] = self.chip(k, 1 - x, i, a).astype(BF)
                self.sy[sx, i, a, :] = self.chip(k, i, 1 - y, b).astype(BF)
        elif n == 2:
            self.s2[s2, 0, a, :] = (self.chip(k, x, 1 - y, a) + self.rx[rx, 1 - y, a, :].astype(F32)).astype(BF)
            self.s2[s2, 1, a, :] = (self.chip(k, 1 - x, y, b) + self.ry[rx, 1 - x, a, :].astype(F32)).astype(BF)
        else:
            first = self.chip(k, x, y, a) + self.rx[rx, y, a, :].astype(F32) + self.r2[r2, 0, a, :].astype(F32)
            second = self.chip(k, x, y, b) + self.ry[rx, x, a, :].astype(F32) + self.r2[r2, 1, a, :].astype(F32)
            first, second = first.astype(BF), second.astype(BF)
            self.put(k, rows, first, second)
            for g in (first, second):
                g = g.astype(F32)
                self.squares[...] += jnp.sum(g * g, 0, keepdims=True)
        if n < 3:
            self.start(n, k, rows)

    def point(self, t, middle, gu, dd):
        for n, k in ((1, t - 1), (3, t - 4)) if middle else ((0, t - 1), (2, t - 3)):
            for low, high, rows in ((0, gu, GU), (gu, gu + dd, DD)):

                @pl.when((k >= low) & (k < high))
                def _():
                    if n:
                        self.stage(n, k, rows)
                    else:
                        self.start(0, k, rows)


def exchange_scratch():
    half = (2, DD // 2, NB)
    return [
        pltpu.VMEM((SRC, 4, 2, DD, NB), BF),
        pltpu.VMEM((RC, 4, DD, NB), BF),
        pltpu.VMEM((SX, *half), BF),
        pltpu.VMEM((SX, *half), BF),
        pltpu.VMEM((RX, *half), BF),
        pltpu.VMEM((RX, *half), BF),
        pltpu.VMEM((S2, *half), BF),
        pltpu.VMEM((R2, *half), BF),
        pltpu.SemaphoreType.DMA((5, RX)),
        pltpu.SemaphoreType.DMA((5, RX)),
    ]


def backward(a, dh, h, gate, up, sq1, wg, wu, wd, layer, collective_id):
    t_, d = a.shape
    ff = wg.shape[2]
    n_gu, n_dd = ff // NB, d // NB
    last = n_gu + n_dd + 3
    inner = h is not None

    def body(*refs):
        if inner:
            a_hbm, dh_ref, h_hbm, wg_ref, wu_ref, wd_ref, rg_ref, ru_ref, rd_ref, sq_ref, o_hbm, abuf, acc, w, io, *refs = refs
        else:
            a_hbm, dh_ref, gate_ref, up_ref, wd_ref, sq1_ref, rg_ref, ru_ref, rd_ref, sum_ref, abuf, sq_ref, sums, sums_got, sums_sem, io, *refs = refs
        at, ht, dgu, *refs = refs
        src = refs[0]
        t = pl.program_id(0)

        def put(k, rows, first, second):
            if rows == GU:
                cols = pl.ds(pl.multiple_of(k * NB, NB), NB)
                rg_ref[:, cols] = first
                ru_ref[:, cols] = second
            else:
                cols = pl.ds(pl.multiple_of((k - n_gu) * NB, NB), NB)
                rd_ref[: DD // 2, cols] = first
                rd_ref[DD // 2 :, cols] = second

        ex = Exchange(*refs, sq_ref, put)

        @pl.when(t == 0)
        def _():
            ex.barrier()
            sq_ref[...] = jnp.zeros_like(sq_ref)
            load = pltpu.make_async_copy(a_hbm, abuf, io)
            load.start()
            if inner:
                for r in tiles(t_, 256):
                    acc[r, :] = jnp.zeros((256, d), F32)
            load.wait()
            for r in tiles(t_, 256):
                at[:, r] = abuf[r, :].T

        ex.point(t, False, n_gu, n_dd)
        slot = lax.rem(t, SRC)

        @pl.when(t < n_gu)
        def _():
            rows = pl.ds(pl.multiple_of(t * NB, NB), NB)
            if inner:
                beside(w, wg_ref, wu_ref)
            for r in tiles(t_, 512):
                if inner:
                    both = dot(abuf[r, :], w[...])
                    gt, u = both[:, :NB], both[:, NB:]
                else:
                    gt, u = gate_ref[r, :], up_ref[r, :]
                dp = dot(dh_ref[r, :], wd_ref[...], 1, 1).astype(BF).astype(F32)
                dgt, dut, sg = hidden_back(dp, gt, u)
                dgu[r, :NB] = dgt
                dgu[r, NB:] = dut
                ht[rows, r] = (sg * u).astype(BF).T
                if inner:
                    acc[r, :] += dot(jnp.concatenate([dgt, dut], 1), w[...], 1, 1)

        def down(i):
            cols = pl.ds(pl.multiple_of((t - n_gu) * NB, NB), NB)
            src[slot, i] = dot(ht[pl.ds(i * 2 * DD, 2 * DD), :], dh_ref[:, cols]).astype(BF).reshape(2, DD, NB)

        ex.point(t, True, n_gu, n_dd)

        @pl.when(t < n_gu)
        def _():
            for i in range(2):
                both = dot(at[pl.ds(i * d // 2, d // 2), :], dgu[...]).astype(BF)
                src[slot, 2 * i : 2 * i + 2, :, : GU // 2, :] = both[:, :NB].reshape(2, 2, GU // 2, NB)
                src[slot, 2 * i : 2 * i + 2, :, GU // 2 : GU, :] = both[:, NB:].reshape(2, 2, GU // 2, NB)

        @pl.when((t >= n_gu) & (t < n_gu + n_dd))
        def _():
            for i in range(4):
                down(i)

        if inner:

            @pl.when(t == n_gu)
            def _():
                pltpu.make_async_copy(h_hbm, abuf, io).start()

            @pl.when(t == n_gu + n_dd)
            def _():
                pltpu.make_async_copy(h_hbm, abuf, io).wait()
                for r in tiles(t_, 256):
                    da = acc[r, :].astype(BF).astype(F32)
                    wide = abuf[r, :].astype(F32)
                    scale = lax.rsqrt(jnp.mean(wide * wide, -1, keepdims=True) + 1e-6)
                    along = jnp.sum(da * wide, -1, keepdims=True) * (scale * scale * scale / d)
                    abuf[r, :] = dh_ref[r, :] + (da * scale - wide * along).astype(BF)

            @pl.when(t == n_gu + n_dd + 1)
            def _():
                pltpu.make_async_copy(abuf, o_hbm, io).start()

            @pl.when(t == last)
            def _():
                pltpu.make_async_copy(abuf, o_hbm, io).wait()

        else:

            @pl.when(t == last)
            def _():
                total = jnp.sum(sq_ref[...] + sq1_ref[...], 1, keepdims=True)
                total = jnp.broadcast_to(total, (8, 128))
                for i, other in enumerate((ex.over_c, ex.over_y, ex.over_x)):
                    sums[i] = total
                    copy = pltpu.make_async_remote_copy(
                        src_ref=sums.at[i], dst_ref=sums_got.at[i], send_sem=sums_sem.at[0, i], recv_sem=sums_sem.at[1, i],
                        device_id={"dp": other}, device_id_type=MESH,
                    )
                    copy.start()
                    copy.wait()
                    total = total + sums_got[i]
                sum_ref[...] = total

    def block(j):
        return jnp.minimum(j, n_gu - 1)

    once = pl.Buffered(1)
    anyw = pl.BlockSpec(memory_space=pl.ANY)
    dh_spec = pl.BlockSpec((t_, d), lambda j: (0, 0), pipeline_mode=once)
    wcol = pl.BlockSpec((None, d, NB), lambda j: (layer, 0, block(j)))
    wrow = pl.BlockSpec((None, NB, d), lambda j: (layer, block(j), 0))
    gcol = pl.BlockSpec((t_, NB), lambda j: (0, block(j)))
    in_specs = [anyw, dh_spec, anyw, wcol, wcol, wrow] if inner else [anyw, dh_spec, gcol, gcol, wrow, whole((1, NB))]
    args = (a, dh, h, wg, wu, wd) if inner else (a, dh, gate, up, wd, sq1)
    shapes = [(d // 8, ff), (d // 8, ff), (ff // 8, d)]
    sums = (1, NB) if inner else (8, 128)
    out_specs = [whole(s) for s in shapes + [sums]] + ([anyw] if inner else [])
    out_shape = [jax.ShapeDtypeStruct(s, BF) for s in shapes] + [jax.ShapeDtypeStruct(sums, F32)]
    out_shape += [jax.ShapeDtypeStruct((t_, d), BF)] if inner else []
    scratch = [pltpu.VMEM((t_, d), BF)]
    if inner:
        scratch += [pltpu.VMEM((t_, d), F32), pltpu.VMEM((d, 2 * NB), BF)]
    else:
        scratch += [pltpu.VMEM((1, NB), F32)] + [pltpu.VMEM((3, 8, 128), F32)] * 2 + [pltpu.SemaphoreType.DMA((2, 3))]
    scratch += [pltpu.SemaphoreType.DMA, pltpu.VMEM((d, t_), BF), pltpu.VMEM((ff, t_), BF), pltpu.VMEM((t_, 2 * NB), BF)]
    return pl.pallas_call(
        body,
        grid=(last + 1,),
        in_specs=in_specs,
        out_specs=out_specs,
        out_shape=out_shape,
        scratch_shapes=scratch + exchange_scratch(),
        compiler_params=pltpu.CompilerParams(
            vmem_limit_bytes=VM, dimension_semantics=("arbitrary",), collective_id=collective_id, has_side_effects=True
        ),
        cost_estimate=cost((16 if inner else 8) * t_ * d * ff, 0),
    )(*args)


def swap(bit):
    return [(i, i ^ bit) for i in range(8)]


def send(t, bit):
    return lax.ppermute(t, "dp", swap(bit))


def place(out, pieces, where, shape):
    rows, n = pieces[0].shape
    count = len(pieces)

    def body(*refs):
        pieces, (o_ref, held, sems) = refs[:count], refs[-3:]
        me = lax.axis_index("dp")
        x, y, c = me // 4, me // 2 % 2, me % 2
        loads = [pltpu.make_async_copy(p, held.at[i], sems.at[0, i]) for i, p in enumerate(pieces)]
        stores = []
        for load in loads:
            load.start()
        for i, (load, (layer, fx, fy, fc)) in enumerate(zip(loads, where)):
            block = (abs(fx - x) * 2 + abs(fy - y)) * 2 + abs(fc - c)
            at = pl.ds(pl.multiple_of(block * rows, rows), rows)
            load.wait()
            stores.append(pltpu.make_async_copy(held.at[i], o_ref.at[layer, at], sems.at[1, i]))
            stores[-1].start()
        for store in stores:
            store.wait()

    args = (*pieces, *(() if out is None else (out,)))
    return pl.pallas_call(
        body,
        in_specs=[pl.BlockSpec(memory_space=pl.ANY)] * len(args),
        out_specs=pl.BlockSpec(memory_space=pl.ANY),
        out_shape=jax.ShapeDtypeStruct(shape, BF),
        scratch_shapes=[pltpu.VMEM((count, rows, n), BF), pltpu.SemaphoreType.DMA((2, count))],
        input_output_aliases={} if out is None else {count: 0},
        cost_estimate=cost(2_000_000_000 * count, 4 * count * rows * n),
        name="place",
    )(*args)


def gathered(owns, shapes, others):
    first = [(own, send(own, 4), send(own, 2), send(own, 1)) for own in owns]
    outs, corners, before = [None] * len(shapes), [], None
    for i, (own, from_x, from_y, from_c) in enumerate(first):
        n, l = divmod(i, 2)
        if i:
            from_x, from_y, outs[before] = lax.optimization_barrier((from_x, from_y, outs[before]))
        corners.append(send(*((from_y, 4) if l else (from_x, 2))))
        pieces = own, from_c, from_x, from_y, send(from_x, 1), send(from_y, 1)
        where = (l, 0, 0, 0), (l, 0, 0, 1), (l, 1, 0, 0), (l, 0, 1, 0), (l, 1, 0, 1), (l, 0, 1, 1)
        outs[n] = place(outs[n], pieces, where, shapes[n])
        before = n
    corners[0], outs[before], *others = lax.optimization_barrier((corners[0], outs[before], *others))
    where = (0, 1, 1, 0), (1, 1, 1, 0), (0, 1, 1, 1), (1, 1, 1, 1)
    for n in range(len(outs)):
        pair = corners[2 * n : 2 * n + 2]
        if n:
            *pair, outs[n - 1] = lax.optimization_barrier((*pair, outs[n - 1]))
        pieces = *pair, *(send(t, 1) for t in pair)
        outs[n] = place(outs[n], pieces, where, shapes[n])
    return outs, others


def moments_of(m, v, g):
    return 0.9 * m + 0.1 * g, 0.95 * v + 0.05 * g * g


def weight_of(w, m, v):
    return (w - 0.02 * (m * lax.rsqrt(v + 1e-8) + 0.1 * w)).astype(BF)


def solution(mesh):
    def step(x, dy, wg, wu, wd, *moments):
        me = lax.axis_index("dp")
        x, dy = x[0], dy[0]

        gate, up, a0, h1, a1 = fwd0(x, wg, wu, wd, 0)
        r_g1, r_u1, r_d1, sq1, dh = backward(a1, dy, h1, None, None, None, wg, wu, wd, 1, 1)
        r_g0, r_u0, r_d0, total = backward(a0, dh, None, gate, up, sq1, wg, wu, wd, 0, 2)
        count = sum(w.size for w in (wg, wu, wd))
        factor = jnp.minimum(1.0, 0.5 * lax.rsqrt(total[0, 0] / count + 1e-30))
        grads = ((r_g0, r_g1), (r_u0, r_u1), (r_d0, r_d1))
        weights, m, v = (wg, wu, wd), moments[:3], moments[3:]
        owns, now = [], factor
        for n, w in enumerate(weights):
            rows = m[n].shape[1]
            for l, g in enumerate(grads[n]):
                own = lax.dynamic_slice(w, (l, me * rows, 0), (1, rows, w.shape[2]))[0]
                own = weight_of(own.astype(F32), *moments_of(m[n][l], v[n][l], g.astype(F32) * now))
                own, now = lax.optimization_barrier((own, now))
                owns.append(own)
        new = [moments_of(m[n], v[n], jnp.stack(grads[n]).astype(F32) * now) for n in range(3)]
        outs, others = gathered(owns, [w.shape for w in weights], [t for pair in zip(*new) for t in pair])
        return (*outs, *others)

    P = jax.sharding.PartitionSpec
    rows = P(None, "dp", None)
    return jax.shard_map(
        step,
        mesh=mesh,
        in_specs=(P(("rep", "dp")),) * 2 + (P(),) * 3 + (rows,) * 6,
        out_specs=(P("rep"),) * 3 + (P("rep", "dp", None),) * 6,
        check_vma=False,
    )
```

```python
import jax
import jax.numpy as jnp
from jax import lax
from jax.experimental import pallas as pl
from jax.experimental.pallas import tpu as pltpu


BF, F32 = jnp.bfloat16, jnp.float32
NB = 256
VM = 64 * 1024 * 1024 - 65536


def dot(a, b, ca=1, cb=0):
    return lax.dot_general(a, b, (((ca,), (cb,)), ((), ())), preferred_element_type=F32)


def normed(h):
    wide = h.astype(F32)
    scale = lax.rsqrt(jnp.mean(wide * wide, -1, keepdims=True) + 1e-6)
    return (wide * scale).astype(BF)


def params():
    return pltpu.CompilerParams(vmem_limit_bytes=VM, dimension_semantics=("arbitrary",))


def whole(shape):
    return pl.BlockSpec(shape, lambda j: (0,) * len(shape))


def cost(mm, by):
    return pl.CostEstimate(flops=mm, bytes_accessed=by, transcendentals=0)


def tiles(t, rt):
    return [pl.ds(i * rt, rt) for i in range(t // rt)]


def beside(ref, one, other):
    n = one.shape[1]
    ref[:, :n] = one[...]
    ref[:, n:] = other[...]


def forward(x, wg, wu, wd):
    t_, d = x.shape
    ff = wg.shape[2]
    n1, rt = ff // NB, 512
    n2 = t_ // rt

    def body(x_hbm, wg_ref, wu_ref, wd_hbm, gate_ref, up_ref, ht_ref, at_hbm, h_ref, xs, a, at, hid, w, wds, sem, wd_sem, at_sem):
        t = pl.program_id(0)
        second = t >= n1 + n2
        wd_load = pltpu.make_async_copy(wd_hbm.at[0], wds, wd_sem)
        early = pl.ds(0, t_ - 256)
        late = pl.ds(t_ - 256, 256)
        at_stores = [pltpu.make_async_copy(at, at_hbm.at[0], at_sem.at[0])]
        at_stores += [pltpu.make_async_copy(at.at[:, c], at_hbm.at[1, :, c], at_sem.at[i]) for i, c in enumerate((early, late))]

        @pl.when(t == 0)
        def _():
            loads = [pltpu.make_async_copy(x_hbm.at[r], xs.at[r], sem.at[i]) for i, r in enumerate(tiles(t_, rt))]
            for load in loads:
                load.start()
            wd_load.start()
            for i, load in enumerate(loads):
                load.wait()
                for r in range(i * rt, (i + 1) * rt, 256):
                    a[pl.ds(r, 256), :] = normed(xs[pl.ds(r, 256), :])

        @pl.when((t < n1) | second)
        def _():
            beside(w, wg_ref, wu_ref)
            j = jnp.where(second, t - n1 - n2, t)
            cols = pl.ds(pl.multiple_of(j * NB, NB), NB)
            part = pl.ds(pl.multiple_of(jnp.minimum(j, t_ // 256 - 1) * 256, 256), 256)
            at[:, part] = a[part, :].T
            for r in tiles(t_, rt):
                both = dot(a[r, :], w[...])
                gate, up = both[:, :NB], both[:, NB:]
                gate_ref[r, :] = gate
                up_ref[r, :] = up
                hidden = (jax.nn.silu(gate) * up).astype(BF)
                hid[r, cols] = hidden
                ht_ref[:, r] = hidden.T

        @pl.when(t == n1)
        def _():
            wd_load.wait()
            at_stores[0].start()

        @pl.when((t >= n1) & (t < n1 + n2))
        def _():
            r = pl.ds(pl.multiple_of((t - n1) * rt, rt), rt)
            h = xs[r, :] + dot(hid[r, :], wds[...]).astype(BF)
            h_ref[...] = h
            a[r, :] = normed(h)

        @pl.when(t == n1 + n2 - 1)
        def _():
            at_stores[0].wait()

        @pl.when(t == 2 * n1 + n2 - 2)
        def _():
            at_stores[1].start()

        @pl.when(t == 2 * n1 + n2 - 1)
        def _():
            at_stores[2].start()
            at_stores[1].wait()
            at_stores[2].wait()

    def layer(j):
        return jnp.where(j < n1 + n2, 0, 1)

    def block(j):
        return jnp.where(j < n1 + n2, jnp.minimum(j, n1 - 1), j - n1 - n2)

    anyw = pl.BlockSpec(memory_space=pl.ANY)
    wcol = pl.BlockSpec((None, d, NB), lambda j: (layer(j), 0, block(j)))
    gcol = pl.BlockSpec((None, t_, NB), lambda j: (layer(j), 0, block(j)))
    hrow = pl.BlockSpec((None, NB, t_), lambda j: (layer(j), block(j), 0))
    return pl.pallas_call(
        body,
        grid=(2 * n1 + n2,),
        in_specs=[anyw, wcol, wcol, anyw],
        out_specs=[gcol, gcol, hrow, anyw, pl.BlockSpec((rt, d), lambda j: (jnp.clip(j - n1, 0, n2 - 1), 0))],
        out_shape=[
            jax.ShapeDtypeStruct((2, t_, ff), F32),
            jax.ShapeDtypeStruct((2, t_, ff), F32),
            jax.ShapeDtypeStruct((2, ff, t_), BF),
            jax.ShapeDtypeStruct((2, d, t_), BF),
            jax.ShapeDtypeStruct((t_, d), BF),
        ],
        scratch_shapes=[
            pltpu.VMEM((t_, d), BF),
            pltpu.VMEM((t_, d), BF),
            pltpu.VMEM((d, t_), BF),
            pltpu.VMEM((t_, ff), BF),
            pltpu.VMEM((d, 2 * NB), BF),
            pltpu.VMEM((ff, d), BF),
            pltpu.SemaphoreType.DMA((n2,)),
            pltpu.SemaphoreType.DMA,
            pltpu.SemaphoreType.DMA((2,)),
        ],
        compiler_params=params(),
        cost_estimate=cost(10 * t_ * d * ff, 0),
        name="forward",
    )(x, wg, wu, wd)


def hidden_back(dh, gate, up):
    s = jax.nn.sigmoid(gate)
    sg = gate * s
    return (dh * up * (s + sg * (1 - s))).astype(BF), (dh * sg).astype(BF)


SLOTS = {True: (4, 5, 2, 6, 2, 4), False: (3, 3, 1, 3, 1, 2)}
MESH = pl.DeviceIdType.MESH
GU, DD = 256, 352


class Exchange:
    def __init__(self, rows, slots, squares, put, src, rc, sx, sy, rx, ry, s2, r2, sent, got):
        self.rows, self.slots = rows, slots
        self.src, self.rc, self.sx, self.sy, self.rx, self.ry, self.s2, self.r2 = src, rc, sx, sy, rx, ry, s2, r2
        self.sent, self.got, self.squares, self.put = sent, got, squares, put
        me = lax.axis_index("dp")
        self.x, self.y, self.c = me // 4, me // 2 % 2, me % 2
        self.over_c, self.over_y, self.over_x = me + 1 - 2 * self.c, me + 2 - 4 * self.y, me + 4 - 8 * self.x

    def barrier(self):
        b = pltpu.get_barrier_semaphore()
        for other in (self.over_c, self.over_y, self.over_x):
            pl.semaphore_signal(b, inc=1, device_id={"dp": other}, device_id_type=MESH)
        pl.semaphore_wait(b, 3)

    def copy(self, n, slot, src, dst, other):
        return pltpu.make_async_remote_copy(
            src_ref=src, dst_ref=dst, send_sem=self.sent.at[n, slot], recv_sem=self.got.at[n, slot],
            device_id={"dp": other}, device_id_type=MESH,
        )

    def copies(self, stage, k):
        rows, h = self.rows, self.rows // 2
        SRC, RC, SX, RX, S2, R2 = self.slots
        if stage == 0:
            s, r = lax.rem(k, SRC), lax.rem(k, RC)
            return [self.copy(0, r, self.src.at[s, :, 1 - self.c, :rows], self.rc.at[r, :, :rows], self.over_c)]
        if stage == 1:
            s, r = lax.rem(k, SX), lax.rem(k, RX)
            return [
                self.copy(1, r, self.sx.at[s, :, :h], self.rx.at[r, :, :h], self.over_x),
                self.copy(2, r, self.sy.at[s, :, :h], self.ry.at[r, :, :h], self.over_y),
            ]
        s, r = lax.rem(k, S2), lax.rem(k, R2)
        return [
            self.copy(3, r, self.s2.at[s, 0, :h], self.r2.at[r, 0, :h], self.over_y),
            self.copy(4, r, self.s2.at[s, 1, :h], self.r2.at[r, 1, :h], self.over_x),
        ]

    def start(self, stage, k):
        for c in self.copies(stage, k):
            c.start()

    def chip(self, k, i, j, part):
        at = i * 2 + j
        return self.src[lax.rem(k, self.slots[0]), at, self.c, part, :].astype(F32) + self.rc[lax.rem(k, self.slots[1]), at, part, :].astype(F32)

    def stage(self, n, k):
        for c in self.copies(n - 1, k):
            c.wait()
        rows, h, x, y = self.rows, self.rows // 2, self.x, self.y
        a, b = slice(0, h), slice(h, rows)
        sx, rx, s2, r2 = (lax.rem(k, m) for m in self.slots[2:])
        if n == 1:
            for i in range(2):
                self.sx[sx, i, a, :] = self.chip(k, 1 - x, i, a).astype(BF)
                self.sy[sx, i, a, :] = self.chip(k, i, 1 - y, b).astype(BF)
        elif n == 2:
            self.s2[s2, 0, a, :] = (self.chip(k, x, 1 - y, a) + self.rx[rx, 1 - y, a, :].astype(F32)).astype(BF)
            self.s2[s2, 1, a, :] = (self.chip(k, 1 - x, y, b) + self.ry[rx, 1 - x, a, :].astype(F32)).astype(BF)
        else:
            first = self.chip(k, x, y, a) + self.rx[rx, y, a, :].astype(F32) + self.r2[r2, 0, a, :].astype(F32)
            second = self.chip(k, x, y, b) + self.ry[rx, x, a, :].astype(F32) + self.r2[r2, 1, a, :].astype(F32)
            first, second = first.astype(BF), second.astype(BF)
            self.put(k, first, second)
            for g in (first, second):
                g = g.astype(F32)
                self.squares[...] += jnp.sum(g * g, 0, keepdims=True)
        if n < 3:
            self.start(n, k)

    def due(self, n, k, when):
        @pl.when(when)
        def _():
            if n:
                self.stage(n, k)
            else:
                self.start(0, k)


def exchange_scratch(rows, slots):
    half = (2, rows // 2, NB)
    SRC, RC, SX, RX, S2, R2 = slots
    shapes = [(SRC, 4, 2, rows, NB), (RC, 4, rows, NB), (SX, *half), (SX, *half), (RX, *half), (RX, *half), (S2, *half), (R2, *half)]
    return [pltpu.VMEM(shape, BF) for shape in shapes] + [pltpu.SemaphoreType.DMA((5, max(slots)))] * 2


def backward(at, dy, h, gate, up, ht, wg, wu, wd):
    _, d, t_ = at.shape
    ff = wg.shape[2]
    n, n_dd = ff // NB, d // NB
    last = 2 * n + 3
    skip = (n + 1) // 2 - n_dd

    def body(
        at_hbm, dy_hbm, h_hbm, g_hbm, u_hbm, ht_hbm, wg_ref, wu_ref, wd_ref, rg_ref, ru_ref, rd_ref, sum_ref,
        dh, hs, acc, w, at, gu, hbuf, dgu, sq, sums, sums_got, sums_sem, at_sem, dh_sem, h_sem, gu_sem, ht_sem, *refs,
    ):
        src, src_d = refs[0], refs[10]
        t = pl.program_id(0)
        inner = t < n

        def put_gu(k, first, second):
            rg_ref[...] = first
            ru_ref[...] = second

        def put_d(k, first, second):
            rd_ref[: DD // 2, :] = first
            rd_ref[DD // 2 :, :] = second

        ex = Exchange(GU, SLOTS[True], sq, put_gu, *refs[:10])
        ex_d = Exchange(DD, SLOTS[False], sq, put_d, *refs[10:])
        at_loads = [pltpu.make_async_copy(at_hbm.at[layer], at, at_sem) for layer in range(2)]
        dh_load = pltpu.make_async_copy(dy_hbm, dh, dh_sem)
        h_load = pltpu.make_async_copy(h_hbm, hs, h_sem)

        def gu_loads(j):
            cols = pl.ds(pl.multiple_of(lax.rem(j, n) * NB, NB), NB)
            return [pltpu.make_async_copy(r.at[1 - j // n, :, cols], gu.at[i], gu_sem.at[i]) for i, r in enumerate((g_hbm, u_hbm))]

        def ht_load():
            rows = pl.ds(pl.multiple_of(lax.rem(t, 2) * 4 * DD, 4 * DD), 4 * DD)
            return pltpu.make_async_copy(ht_hbm.at[1 - t // n, rows], hbuf, ht_sem)

        @pl.when(t == 0)
        def _():
            dh_load.start()
            for load in gu_loads(0):
                load.start()
            at_loads[1].start()
            sq[...] = jnp.zeros_like(sq)
            for r in tiles(t_, 256):
                acc[r, :] = jnp.zeros((256, d), F32)
            ex.barrier()
            dh_load.wait()

        pair, even = t // 2, lax.rem(t, 2) == 0
        odd = lax.rem(t, 2) == 1
        start = 2 * (n_dd + skip)
        making_d = (t < 2 * n_dd) | ((t >= start) & (t < start + 2 * n_dd))
        column = jnp.where(t < start, pair, pair - n_dd - skip)

        @pl.when(making_d)
        def _():
            ht_load().start()

        def due_d(stage, later, when):
            k = pair - later
            ex_d.due(stage, k, when & (k >= 0) & (k < n_dd))
            ex_d.due(stage, k - skip, when & (k >= n_dd + skip) & (k < 2 * n_dd + skip))

        ex.due(0, t - 1, (t >= 1) & (t <= 2 * n))
        due_d(0, 1, even)
        ex.due(2, t - 3, (t >= 3) & (t <= 2 * n + 2))
        due_d(2, 2, even)

        @pl.when(t == n)
        def _():
            at_loads[0].start()
            h_load.wait()
            for r in tiles(t_, 256):
                da = acc[r, :].astype(BF).astype(F32)
                wide = hs[r, :].astype(F32)
                scale = lax.rsqrt(jnp.mean(wide * wide, -1, keepdims=True) + 1e-6)
                along = jnp.sum(da * wide, -1, keepdims=True) * (scale * scale * scale / d)
                dh[r, :] = dh[r, :] + (da * scale - wide * along).astype(BF)

        def hidden_units(inner):
            for load in gu_loads(t):
                load.wait()
            if inner:
                beside(w, wg_ref, wu_ref)
            for r in tiles(t_, 512):
                dp = dot(dh[r, :], wd_ref[...], 1, 1).astype(BF).astype(F32)
                dgt, dut = hidden_back(dp, gu[0, r, :], gu[1, r, :])
                dgu[r, :NB] = dgt
                dgu[r, NB:] = dut
                if inner:
                    acc[r, :] += dot(jnp.concatenate([dgt, dut], 1), w[...], 1, 1)

        @pl.when(inner)
        def _():
            hidden_units(True)

        @pl.when((t >= n) & (t < 2 * n))
        def _():
            hidden_units(False)

        @pl.when(t < 2 * n - 1)
        def _():
            for load in gu_loads(t + 1):
                load.start()

        ex.due(1, t - 1, (t >= 1) & (t <= 2 * n))
        due_d(1, 1, even)
        ex.due(3, t - 4, (t >= 4) & (t <= 2 * n + 3))
        due_d(3, 2, odd)

        @pl.when(t == 0)
        def _():
            h_load.start()
            at_loads[1].wait()

        @pl.when(t == n)
        def _():
            at_loads[0].wait()

        @pl.when(t < 2 * n)
        def _():
            slot = lax.rem(t, SLOTS[True][0])
            for i in range(2):
                both = dot(at[pl.ds(i * d // 2, d // 2), :], dgu[...]).astype(BF)
                src[slot, 2 * i : 2 * i + 2, :, : GU // 2, :] = both[:, :NB].reshape(2, 2, GU // 2, NB)
                src[slot, 2 * i : 2 * i + 2, :, GU // 2 :, :] = both[:, NB:].reshape(2, 2, GU // 2, NB)

        @pl.when(making_d)
        def _():
            ht_load().wait()
            slot = lax.rem(jnp.where(t < start, pair, pair - skip), SLOTS[False][0])
            cols = pl.ds(pl.multiple_of(column * NB, NB), NB)
            for i in range(2):
                rows = pl.ds(i * 2 * DD, 2 * DD)
                src_d[slot, 2 * lax.rem(t, 2) + i] = dot(hbuf[rows, :], dh[:, cols]).astype(BF).reshape(2, DD, NB)

        @pl.when(t == last)
        def _():
            total = jnp.broadcast_to(jnp.sum(sq[...], 1, keepdims=True), (8, 128))
            for i, other in enumerate((ex.over_c, ex.over_y, ex.over_x)):
                sums[i] = total
                copy = pltpu.make_async_remote_copy(
                    src_ref=sums.at[i], dst_ref=sums_got.at[i], send_sem=sums_sem.at[0, i], recv_sem=sums_sem.at[1, i],
                    device_id={"dp": other}, device_id_type=MESH,
                )
                copy.start()
                copy.wait()
                total = total + sums_got[i]
            sum_ref[...] = total

    def tick(j):
        return jnp.minimum(j, 2 * n - 1)

    def gu_out(j):
        k = jnp.clip(j - 4, 0, 2 * n - 1)
        return (1 - k // n, 0, k % n)

    def d_out(j):
        k = jnp.maximum(j - 5, 0) // 2
        k = jnp.where(k < n_dd + skip, jnp.minimum(k, n_dd - 1), jnp.minimum(k - skip, 2 * n_dd - 1))
        return (1 - k // n_dd, 0, k % n_dd)

    anyw = pl.BlockSpec(memory_space=pl.ANY)
    wcol = pl.BlockSpec((None, d, NB), lambda j: (1, 0, jnp.minimum(j, n - 1)))
    wrow = pl.BlockSpec((None, NB, d), lambda j: (1 - tick(j) // n, tick(j) % n, 0))
    out_gu = pl.BlockSpec((None, d // 8, NB), gu_out)
    return pl.pallas_call(
        body,
        grid=(last + 1,),
        in_specs=[anyw] * 6 + [wcol, wcol, wrow],
        out_specs=[out_gu, out_gu, pl.BlockSpec((None, ff // 8, NB), d_out), whole((8, 128))],
        out_shape=[
            jax.ShapeDtypeStruct((2, d // 8, ff), BF),
            jax.ShapeDtypeStruct((2, d // 8, ff), BF),
            jax.ShapeDtypeStruct((2, ff // 8, d), BF),
            jax.ShapeDtypeStruct((8, 128), F32),
        ],
        scratch_shapes=[
            pltpu.VMEM((t_, d), BF),
            pltpu.VMEM((t_, d), BF),
            pltpu.VMEM((t_, d), F32),
            pltpu.VMEM((d, 2 * NB), BF),
            pltpu.VMEM((d, t_), BF),
            pltpu.VMEM((2, t_, NB), F32),
            pltpu.VMEM((4 * DD, t_), BF),
            pltpu.VMEM((t_, 2 * NB), BF),
            pltpu.VMEM((1, NB), F32),
            pltpu.VMEM((3, 8, 128), F32),
            pltpu.VMEM((3, 8, 128), F32),
            pltpu.SemaphoreType.DMA((2, 3)),
            pltpu.SemaphoreType.DMA,
            pltpu.SemaphoreType.DMA,
            pltpu.SemaphoreType.DMA,
            pltpu.SemaphoreType.DMA((2,)),
            pltpu.SemaphoreType.DMA,
        ]
        + exchange_scratch(GU, SLOTS[True])
        + exchange_scratch(DD, SLOTS[False]),
        compiler_params=pltpu.CompilerParams(
            vmem_limit_bytes=VM, dimension_semantics=("arbitrary",), collective_id=1, has_side_effects=True
        ),
        cost_estimate=cost(20 * t_ * d * ff, 0),
        name="backward",
    )(at, dy, h, gate, up, ht, wg, wu, wd)


def swap(bit):
    return [(i, i ^ bit) for i in range(8)]


def send(t, bit):
    return lax.ppermute(t, "dp", swap(bit))


def place(out, pieces, where, shape):
    rows, n = pieces[0].shape
    count = len(pieces)

    def body(*refs):
        pieces, (o_ref, held, sems) = refs[:count], refs[-3:]
        me = lax.axis_index("dp")
        x, y, c = me // 4, me // 2 % 2, me % 2
        loads = [pltpu.make_async_copy(p, held.at[i], sems.at[0, i]) for i, p in enumerate(pieces)]
        stores = []
        for load in loads:
            load.start()
        for i, (load, (layer, fx, fy, fc)) in enumerate(zip(loads, where)):
            block = (abs(fx - x) * 2 + abs(fy - y)) * 2 + abs(fc - c)
            at = pl.ds(pl.multiple_of(block * rows, rows), rows)
            load.wait()
            stores.append(pltpu.make_async_copy(held.at[i], o_ref.at[layer, at], sems.at[1, i]))
            stores[-1].start()
        for store in stores:
            store.wait()

    args = (*pieces, *(() if out is None else (out,)))
    return pl.pallas_call(
        body,
        in_specs=[pl.BlockSpec(memory_space=pl.ANY)] * len(args),
        out_specs=pl.BlockSpec(memory_space=pl.ANY),
        out_shape=jax.ShapeDtypeStruct(shape, BF),
        scratch_shapes=[pltpu.VMEM((count, rows, n), BF), pltpu.SemaphoreType.DMA((2, count))],
        input_output_aliases={} if out is None else {count: 0},
        cost_estimate=cost(2_000_000_000 * count, 4 * count * rows * n),
        name="place",
    )(*args)


def gathered(owns, shapes, others):
    first = [(own, send(own, 4), send(own, 2), send(own, 1)) for own in owns]
    outs, corners, before = [None] * len(shapes), [], None
    for i, (own, from_x, from_y, from_c) in enumerate(first):
        n, l = divmod(i, 2)
        if i:
            from_x, from_y, outs[before] = lax.optimization_barrier((from_x, from_y, outs[before]))
        corners.append(send(*((from_y, 4) if l else (from_x, 2))))
        pieces = own, from_c, from_x, from_y, send(from_x, 1), send(from_y, 1)
        where = (l, 0, 0, 0), (l, 0, 0, 1), (l, 1, 0, 0), (l, 0, 1, 0), (l, 1, 0, 1), (l, 0, 1, 1)
        outs[n] = place(outs[n], pieces, where, shapes[n])
        before = n
    corners[0], outs[before], *others = lax.optimization_barrier((corners[0], outs[before], *others))
    where = (0, 1, 1, 0), (1, 1, 1, 0), (0, 1, 1, 1), (1, 1, 1, 1)
    for n in range(len(outs)):
        pair = corners[2 * n : 2 * n + 2]
        if n:
            *pair, outs[n - 1] = lax.optimization_barrier((*pair, outs[n - 1]))
        pieces = *pair, *(send(t, 1) for t in pair)
        outs[n] = place(outs[n], pieces, where, shapes[n])
    return outs, others


def moments_of(m, v, g):
    return 0.9 * m + 0.1 * g, 0.95 * v + 0.05 * g * g


def weight_of(w, m, v):
    return (w - 0.02 * (m * lax.rsqrt(v + 1e-8) + 0.1 * w)).astype(BF)


def solution(mesh):
    def step(x, dy, wg, wu, wd, *moments):
        me = lax.axis_index("dp")
        x, dy = x[0], dy[0]

        gate, up, ht, at, h = forward(x, wg, wu, wd)
        *grads, total = backward(at, dy, h, gate, up, ht, wg, wu, wd)
        count = sum(w.size for w in (wg, wu, wd))
        factor = jnp.minimum(1.0, 0.5 * lax.rsqrt(total[0, 0] / count + 1e-30))
        weights, m, v = (wg, wu, wd), moments[:3], moments[3:]
        owns, now = [], factor
        for n, w in enumerate(weights):
            rows = m[n].shape[1]
            for l in range(w.shape[0]):
                own = lax.dynamic_slice(w, (l, me * rows, 0), (1, rows, w.shape[2]))[0]
                own = weight_of(own.astype(F32), *moments_of(m[n][l], v[n][l], grads[n][l].astype(F32) * now))
                own, now = lax.optimization_barrier((own, now))
                owns.append(own)
        new = [moments_of(m[n], v[n], grads[n].astype(F32) * now) for n in range(3)]
        outs, others = gathered(owns, [w.shape for w in weights], [t for pair in zip(*new) for t in pair])
        return (*outs, *others)

    P = jax.sharding.PartitionSpec
    rows = P(None, "dp", None)
    return jax.shard_map(
        step,
        mesh=mesh,
        in_specs=(P(("rep", "dp")),) * 2 + (P(),) * 3 + (rows,) * 6,
        out_specs=(P("rep"),) * 3 + (P("rep", "dp", None),) * 6,
        check_vma=False,
    )
```

```python
import jax
import jax.numpy as jnp
from jax import lax
from jax.experimental import pallas as pl
from jax.experimental.pallas import tpu as pltpu


BF, F32 = jnp.bfloat16, jnp.float32
NB = 256
VM = 64 * 1024 * 1024 - 65536


def dot(a, b, ca=1, cb=0):
    return lax.dot_general(a, b, (((ca,), (cb,)), ((), ())), preferred_element_type=F32)


def normed(h):
    wide = h.astype(F32)
    scale = lax.rsqrt(jnp.mean(wide * wide, -1, keepdims=True) + 1e-6)
    return (wide * scale).astype(BF)


def params():
    return pltpu.CompilerParams(vmem_limit_bytes=VM, dimension_semantics=("arbitrary",))


def whole(shape):
    return pl.BlockSpec(shape, lambda j: (0,) * len(shape))


def cost(mm, by):
    return pl.CostEstimate(flops=mm, bytes_accessed=by, transcendentals=0)


def tiles(t, rt):
    return [pl.ds(i * rt, rt) for i in range(t // rt)]


def beside(ref, one, other):
    n = one.shape[1]
    ref[:, :n] = one[...]
    ref[:, n:] = other[...]


def forward(x, wg, wu, wd):
    t_, d = x.shape
    ff = wg.shape[2]
    n1, rt = ff // NB, 512
    n2 = t_ // rt

    def body(x_hbm, wg_ref, wu_ref, wd_hbm, gate_ref, up_ref, ht_ref, at_hbm, h_ref, xs, a, at, hid, w, wds, sem, wd_sem, at_sem):
        t = pl.program_id(0)
        second = t >= n1 + n2
        wd_load = pltpu.make_async_copy(wd_hbm.at[0], wds, wd_sem)
        early = pl.ds(0, t_ - 256)
        late = pl.ds(t_ - 256, 256)
        at_stores = [pltpu.make_async_copy(at, at_hbm.at[0], at_sem.at[0])]
        at_stores += [pltpu.make_async_copy(at.at[:, c], at_hbm.at[1, :, c], at_sem.at[i]) for i, c in enumerate((early, late))]

        @pl.when(t == 0)
        def _():
            loads = [pltpu.make_async_copy(x_hbm.at[r], xs.at[r], sem.at[i]) for i, r in enumerate(tiles(t_, rt))]
            for load in loads:
                load.start()
            wd_load.start()
            for i, load in enumerate(loads):
                load.wait()
                for r in range(i * rt, (i + 1) * rt, 256):
                    a[pl.ds(r, 256), :] = normed(xs[pl.ds(r, 256), :])

        @pl.when((t < n1) | second)
        def _():
            beside(w, wg_ref, wu_ref)
            j = jnp.where(second, t - n1 - n2, t)
            cols = pl.ds(pl.multiple_of(j * NB, NB), NB)
            part = pl.ds(pl.multiple_of(jnp.minimum(j, t_ // 256 - 1) * 256, 256), 256)
            at[:, part] = a[part, :].T
            for r in tiles(t_, rt):
                both = dot(a[r, :], w[...])
                gate, up = both[:, :NB], both[:, NB:]
                gate_ref[r, :] = gate
                up_ref[r, :] = up
                hidden = (jax.nn.silu(gate) * up).astype(BF)
                hid[r, cols] = hidden
                ht_ref[:, r] = hidden.T

        @pl.when(t == n1)
        def _():
            wd_load.wait()
            at_stores[0].start()

        @pl.when((t >= n1) & (t < n1 + n2))
        def _():
            r = pl.ds(pl.multiple_of((t - n1) * rt, rt), rt)
            h = xs[r, :] + dot(hid[r, :], wds[...]).astype(BF)
            h_ref[...] = h
            a[r, :] = normed(h)

        @pl.when(t == n1 + n2 - 1)
        def _():
            at_stores[0].wait()

        @pl.when(t == 2 * n1 + n2 - 2)
        def _():
            at_stores[1].start()

        @pl.when(t == 2 * n1 + n2 - 1)
        def _():
            at_stores[2].start()
            at_stores[1].wait()
            at_stores[2].wait()

    def layer(j):
        return jnp.where(j < n1 + n2, 0, 1)

    def block(j):
        return jnp.where(j < n1 + n2, jnp.minimum(j, n1 - 1), j - n1 - n2)

    anyw = pl.BlockSpec(memory_space=pl.ANY)
    wcol = pl.BlockSpec((None, d, NB), lambda j: (layer(j), 0, block(j)))
    gcol = pl.BlockSpec((None, t_, NB), lambda j: (layer(j), 0, block(j)))
    hrow = pl.BlockSpec((None, NB, t_), lambda j: (layer(j), block(j), 0))
    return pl.pallas_call(
        body,
        grid=(2 * n1 + n2,),
        in_specs=[anyw, wcol, wcol, anyw],
        out_specs=[gcol, gcol, hrow, anyw, pl.BlockSpec((rt, d), lambda j: (jnp.clip(j - n1, 0, n2 - 1), 0))],
        out_shape=[
            jax.ShapeDtypeStruct((2, t_, ff), F32),
            jax.ShapeDtypeStruct((2, t_, ff), F32),
            jax.ShapeDtypeStruct((2, ff, t_), BF),
            jax.ShapeDtypeStruct((2, d, t_), BF),
            jax.ShapeDtypeStruct((t_, d), BF),
        ],
        scratch_shapes=[
            pltpu.VMEM((t_, d), BF),
            pltpu.VMEM((t_, d), BF),
            pltpu.VMEM((d, t_), BF),
            pltpu.VMEM((t_, ff), BF),
            pltpu.VMEM((d, 2 * NB), BF),
            pltpu.VMEM((ff, d), BF),
            pltpu.SemaphoreType.DMA((n2,)),
            pltpu.SemaphoreType.DMA,
            pltpu.SemaphoreType.DMA((2,)),
        ],
        compiler_params=params(),
        cost_estimate=cost(10 * t_ * d * ff, 0),
        name="forward",
    )(x, wg, wu, wd)


def hidden_back(dh, gate, up):
    s = jax.nn.sigmoid(gate)
    sg = gate * s
    return (dh * up * (s + sg * (1 - s))).astype(BF), (dh * sg).astype(BF)


SLOTS = {True: (4, 5, 2, 6, 2, 4), False: (3, 3, 1, 3, 1, 2)}
MESH = pl.DeviceIdType.MESH
GU, DD = 256, 352


class Exchange:
    def __init__(self, rows, slots, squares, put, src, rc, sx, sy, rx, ry, s2, r2, sent, got):
        self.rows, self.slots = rows, slots
        self.src, self.rc, self.sx, self.sy, self.rx, self.ry, self.s2, self.r2 = src, rc, sx, sy, rx, ry, s2, r2
        self.sent, self.got, self.squares, self.put = sent, got, squares, put
        me = lax.axis_index("dp")
        self.me, self.others = me, [lax.rem(me + i, 8) for i in range(1, 8)]
        self.x, self.y, self.c = me // 4, me // 2 % 2, me % 2
        self.over_c, self.over_y, self.over_x = me + 1 - 2 * self.c, me + 2 - 4 * self.y, me + 4 - 8 * self.x

    def barrier(self):
        b = pltpu.get_barrier_semaphore()
        for other in self.others:
            pl.semaphore_signal(b, inc=1, device_id={"dp": other}, device_id_type=MESH)
        pl.semaphore_wait(b, len(self.others))

    def copy(self, n, slot, src, dst, other):
        return pltpu.make_async_remote_copy(
            src_ref=src, dst_ref=dst, send_sem=self.sent.at[n, slot], recv_sem=self.got.at[n, slot],
            device_id={"dp": other}, device_id_type=MESH,
        )

    def copies(self, stage, k):
        rows, h = self.rows, self.rows // 2
        SRC, RC, SX, RX, S2, R2 = self.slots
        if stage == 0:
            s, r = lax.rem(k, SRC), lax.rem(k, RC)
            return [self.copy(0, r, self.src.at[s, :, 1 - self.c, :rows], self.rc.at[r, :, :rows], self.over_c)]
        if stage == 1:
            s, r = lax.rem(k, SX), lax.rem(k, RX)
            return [
                self.copy(1, r, self.sx.at[s, :, :h], self.rx.at[r, :, :h], self.over_x),
                self.copy(2, r, self.sy.at[s, :, :h], self.ry.at[r, :, :h], self.over_y),
            ]
        s, r = lax.rem(k, S2), lax.rem(k, R2)
        return [
            self.copy(3, r, self.s2.at[s, 0, :h], self.r2.at[r, 0, :h], self.over_y),
            self.copy(4, r, self.s2.at[s, 1, :h], self.r2.at[r, 1, :h], self.over_x),
        ]

    def start(self, stage, k):
        for c in self.copies(stage, k):
            c.start()

    def chip(self, k, i, j, part):
        at = i * 2 + j
        return self.src[lax.rem(k, self.slots[0]), at, self.c, part, :].astype(F32) + self.rc[lax.rem(k, self.slots[1]), at, part, :].astype(F32)

    def stage(self, n, k):
        for c in self.copies(n - 1, k):
            c.wait()
        rows, h, x, y = self.rows, self.rows // 2, self.x, self.y
        a, b = slice(0, h), slice(h, rows)
        sx, rx, s2, r2 = (lax.rem(k, m) for m in self.slots[2:])
        if n == 1:
            for i in range(2):
                self.sx[sx, i, a, :] = self.chip(k, 1 - x, i, a).astype(BF)
                self.sy[sx, i, a, :] = self.chip(k, i, 1 - y, b).astype(BF)
        elif n == 2:
            self.s2[s2, 0, a, :] = (self.chip(k, x, 1 - y, a) + self.rx[rx, 1 - y, a, :].astype(F32)).astype(BF)
            self.s2[s2, 1, a, :] = (self.chip(k, 1 - x, y, b) + self.ry[rx, 1 - x, a, :].astype(F32)).astype(BF)
        else:
            first = self.chip(k, x, y, a) + self.rx[rx, y, a, :].astype(F32) + self.r2[r2, 0, a, :].astype(F32)
            second = self.chip(k, x, y, b) + self.ry[rx, x, a, :].astype(F32) + self.r2[r2, 1, a, :].astype(F32)
            first, second = first.astype(BF), second.astype(BF)
            self.put(k, first, second)
            for g in (first, second):
                g = g.astype(F32)
                self.squares[...] += jnp.sum(g * g, 0, keepdims=True)
        if n < 3:
            self.start(n, k)

    def due(self, n, k, when):
        @pl.when(when)
        def _():
            if n:
                self.stage(n, k)
            else:
                self.start(0, k)


def exchange_scratch(rows, slots):
    half = (2, rows // 2, NB)
    SRC, RC, SX, RX, S2, R2 = slots
    shapes = [(SRC, 4, 2, rows, NB), (RC, 4, rows, NB), (SX, *half), (SX, *half), (RX, *half), (RX, *half), (S2, *half), (R2, *half)]
    return [pltpu.VMEM(shape, BF) for shape in shapes] + [pltpu.SemaphoreType.DMA((5, max(slots)))] * 2


def backward(at, dy, h, gate, up, ht, wg, wu, wd):
    _, d, t_ = at.shape
    ff = wg.shape[2]
    n, n_dd = ff // NB, d // NB
    last = 2 * n + 3
    count = wg.size + wu.size + wd.size
    skip = (n + 1) // 2 - n_dd

    def body(
        at_hbm, dy_hbm, h_hbm, g_hbm, u_hbm, ht_hbm, wg_ref, wu_ref, wd_ref, rg_ref, ru_ref, rd_ref, factor_ref,
        dh, hs, acc, w, at, gu, hbuf, dgu, sq, sums, sums_got, sums_sem, at_sem, dh_sem, h_sem, gu_sem, ht_sem, *refs,
    ):
        src, src_d = refs[0], refs[10]
        t = pl.program_id(0)
        inner = t < n

        def put_gu(k, first, second):
            rg_ref[...] = first
            ru_ref[...] = second

        def put_d(k, first, second):
            rd_ref[: DD // 2, :] = first
            rd_ref[DD // 2 :, :] = second

        ex = Exchange(GU, SLOTS[True], sq, put_gu, *refs[:10])
        ex_d = Exchange(DD, SLOTS[False], sq, put_d, *refs[10:])
        at_loads = [pltpu.make_async_copy(at_hbm.at[layer], at, at_sem) for layer in range(2)]
        dh_load = pltpu.make_async_copy(dy_hbm, dh, dh_sem)
        h_load = pltpu.make_async_copy(h_hbm, hs, h_sem)

        def gu_loads(j):
            cols = pl.ds(pl.multiple_of(lax.rem(j, n) * NB, NB), NB)
            return [pltpu.make_async_copy(r.at[1 - j // n, :, cols], gu.at[i], gu_sem.at[i]) for i, r in enumerate((g_hbm, u_hbm))]

        def ht_load():
            rows = pl.ds(pl.multiple_of(lax.rem(t, 2) * 4 * DD, 4 * DD), 4 * DD)
            return pltpu.make_async_copy(ht_hbm.at[1 - t // n, rows], hbuf, ht_sem)

        @pl.when(t == 0)
        def _():
            dh_load.start()
            for load in gu_loads(0):
                load.start()
            at_loads[1].start()
            sq[...] = jnp.zeros_like(sq)
            for r in tiles(t_, 256):
                acc[r, :] = jnp.zeros((256, d), F32)
            ex.barrier()
            dh_load.wait()

        pair, even = t // 2, lax.rem(t, 2) == 0
        odd = lax.rem(t, 2) == 1
        start = 2 * (n_dd + skip)
        making_d = (t < 2 * n_dd) | ((t >= start) & (t < start + 2 * n_dd))
        column = jnp.where(t < start, pair, pair - n_dd - skip)

        @pl.when(making_d)
        def _():
            ht_load().start()

        def due_d(stage, later, when):
            k = pair - later
            ex_d.due(stage, k, when & (k >= 0) & (k < n_dd))
            ex_d.due(stage, k - skip, when & (k >= n_dd + skip) & (k < 2 * n_dd + skip))

        ex.due(0, t - 1, (t >= 1) & (t <= 2 * n))
        due_d(0, 1, even)
        ex.due(2, t - 3, (t >= 3) & (t <= 2 * n + 2))
        due_d(2, 2, even)

        @pl.when(t == n)
        def _():
            at_loads[0].start()
            h_load.wait()
            for r in tiles(t_, 256):
                da = acc[r, :].astype(BF).astype(F32)
                wide = hs[r, :].astype(F32)
                scale = lax.rsqrt(jnp.mean(wide * wide, -1, keepdims=True) + 1e-6)
                along = jnp.sum(da * wide, -1, keepdims=True) * (scale * scale * scale / d)
                dh[r, :] = dh[r, :] + (da * scale - wide * along).astype(BF)

        def hidden_units(inner):
            for load in gu_loads(t):
                load.wait()
            if inner:
                beside(w, wg_ref, wu_ref)
            for r in tiles(t_, 512):
                dp = dot(dh[r, :], wd_ref[...], 1, 1).astype(BF).astype(F32)
                dgt, dut = hidden_back(dp, gu[0, r, :], gu[1, r, :])
                dgu[r, :NB] = dgt
                dgu[r, NB:] = dut
                if inner:
                    acc[r, :] += dot(jnp.concatenate([dgt, dut], 1), w[...], 1, 1)

        @pl.when(inner)
        def _():
            hidden_units(True)

        @pl.when((t >= n) & (t < 2 * n))
        def _():
            hidden_units(False)

        @pl.when(t < 2 * n - 1)
        def _():
            for load in gu_loads(t + 1):
                load.start()

        ex.due(1, t - 1, (t >= 1) & (t <= 2 * n))
        due_d(1, 1, even)
        ex.due(3, t - 4, (t >= 4) & (t <= 2 * n + 3))
        due_d(3, 2, odd)

        @pl.when(t == 0)
        def _():
            h_load.start()
            at_loads[1].wait()

        @pl.when(t == n)
        def _():
            at_loads[0].wait()

        @pl.when(t < 2 * n)
        def _():
            slot = lax.rem(t, SLOTS[True][0])
            for i in range(2):
                both = dot(at[pl.ds(i * d // 2, d // 2), :], dgu[...]).astype(BF)
                src[slot, 2 * i : 2 * i + 2, :, : GU // 2, :] = both[:, :NB].reshape(2, 2, GU // 2, NB)
                src[slot, 2 * i : 2 * i + 2, :, GU // 2 :, :] = both[:, NB:].reshape(2, 2, GU // 2, NB)

        @pl.when(making_d)
        def _():
            ht_load().wait()
            slot = lax.rem(jnp.where(t < start, pair, pair - skip), SLOTS[False][0])
            cols = pl.ds(pl.multiple_of(column * NB, NB), NB)
            for i in range(2):
                rows = pl.ds(i * 2 * DD, 2 * DD)
                src_d[slot, 2 * lax.rem(t, 2) + i] = dot(hbuf[rows, :], dh[:, cols]).astype(BF).reshape(2, DD, NB)

        @pl.when(t == last)
        def _():
            own = jnp.broadcast_to(jnp.sum(sq[...], 1, keepdims=True), (8, 128))
            sums[...] = own
            sums_got[ex.me] = own
            copies = [
                pltpu.make_async_remote_copy(
                    src_ref=sums, dst_ref=sums_got.at[ex.me], send_sem=sums_sem.at[0, i], recv_sem=sums_sem.at[1, i],
                    device_id={"dp": other}, device_id_type=MESH,
                )
                for i, other in enumerate(ex.others)
            ]
            for copy in copies:
                copy.start()
            for copy in copies:
                copy.wait()
            total = sums_got[0]
            for i in range(1, 8):
                total = total + sums_got[i]
            factor = jnp.minimum(1.0, 0.5 * lax.rsqrt(total / count + 1e-30))
            factor_ref[...] = factor[:1, :1]

    def tick(j):
        return jnp.minimum(j, 2 * n - 1)

    def gu_out(j):
        k = jnp.clip(j - 4, 0, 2 * n - 1)
        return (1 - k // n, 0, k % n)

    def d_out(j):
        k = jnp.maximum(j - 5, 0) // 2
        k = jnp.where(k < n_dd + skip, jnp.minimum(k, n_dd - 1), jnp.minimum(k - skip, 2 * n_dd - 1))
        return (1 - k // n_dd, 0, k % n_dd)

    anyw = pl.BlockSpec(memory_space=pl.ANY)
    wcol = pl.BlockSpec((None, d, NB), lambda j: (1, 0, jnp.minimum(j, n - 1)))
    wrow = pl.BlockSpec((None, NB, d), lambda j: (1 - tick(j) // n, tick(j) % n, 0))
    out_gu = pl.BlockSpec((None, d // 8, NB), gu_out)
    return pl.pallas_call(
        body,
        grid=(last + 1,),
        in_specs=[anyw] * 6 + [wcol, wcol, wrow],
        out_specs=[out_gu, out_gu, pl.BlockSpec((None, ff // 8, NB), d_out), whole((1, 1))],
        out_shape=[
            jax.ShapeDtypeStruct((2, d // 8, ff), BF),
            jax.ShapeDtypeStruct((2, d // 8, ff), BF),
            jax.ShapeDtypeStruct((2, ff // 8, d), BF),
            jax.ShapeDtypeStruct((1, 1), F32),
        ],
        scratch_shapes=[
            pltpu.VMEM((t_, d), BF),
            pltpu.VMEM((t_, d), BF),
            pltpu.VMEM((t_, d), F32),
            pltpu.VMEM((d, 2 * NB), BF),
            pltpu.VMEM((d, t_), BF),
            pltpu.VMEM((2, t_, NB), F32),
            pltpu.VMEM((4 * DD, t_), BF),
            pltpu.VMEM((t_, 2 * NB), BF),
            pltpu.VMEM((1, NB), F32),
            pltpu.VMEM((8, 128), F32),
            pltpu.VMEM((8, 8, 128), F32),
            pltpu.SemaphoreType.DMA((2, 7)),
            pltpu.SemaphoreType.DMA,
            pltpu.SemaphoreType.DMA,
            pltpu.SemaphoreType.DMA,
            pltpu.SemaphoreType.DMA((2,)),
            pltpu.SemaphoreType.DMA,
        ]
        + exchange_scratch(GU, SLOTS[True])
        + exchange_scratch(DD, SLOTS[False]),
        compiler_params=pltpu.CompilerParams(
            vmem_limit_bytes=VM, dimension_semantics=("arbitrary",), collective_id=1, has_side_effects=True
        ),
        cost_estimate=cost(20 * t_ * d * ff, 0),
        name="backward",
    )(at, dy, h, gate, up, ht, wg, wu, wd)


def swap(bit):
    return [(i, i ^ bit) for i in range(8)]


def send(t, bit):
    return lax.ppermute(t, "dp", swap(bit))


def place(out, pieces, where, shape):
    rows, n = pieces[0].shape
    count = len(pieces)

    def body(*refs):
        pieces, (o_ref, held, sems) = refs[:count], refs[-3:]
        me = lax.axis_index("dp")
        x, y, c = me // 4, me // 2 % 2, me % 2
        loads = [pltpu.make_async_copy(p, held.at[i], sems.at[0, i]) for i, p in enumerate(pieces)]
        stores = []
        for load in loads:
            load.start()
        for i, (load, (layer, fx, fy, fc)) in enumerate(zip(loads, where)):
            block = (abs(fx - x) * 2 + abs(fy - y)) * 2 + abs(fc - c)
            at = pl.ds(pl.multiple_of(block * rows, rows), rows)
            load.wait()
            stores.append(pltpu.make_async_copy(held.at[i], o_ref.at[layer, at], sems.at[1, i]))
            stores[-1].start()
        for store in stores:
            store.wait()

    args = (*pieces, *(() if out is None else (out,)))
    return pl.pallas_call(
        body,
        in_specs=[pl.BlockSpec(memory_space=pl.ANY)] * len(args),
        out_specs=pl.BlockSpec(memory_space=pl.ANY),
        out_shape=jax.ShapeDtypeStruct(shape, BF),
        scratch_shapes=[pltpu.VMEM((count, rows, n), BF), pltpu.SemaphoreType.DMA((2, count))],
        input_output_aliases={} if out is None else {count: 0},
        compiler_params=pltpu.CompilerParams(vmem_limit_bytes=VM),
        cost_estimate=cost(2_000_000_000 * count, 4 * count * rows * n),
        name="place",
    )(*args)


def gathered(owns, shapes, others):
    first = [(own, send(own, 4), send(own, 2), send(own, 1)) for own in owns]
    outs, corners, before = [None] * len(shapes), [], None
    for i, (own, from_x, from_y, from_c) in enumerate(first):
        n, l = divmod(i, 2)
        if i:
            from_x, from_y, outs[before] = lax.optimization_barrier((from_x, from_y, outs[before]))
        corners.append(send(*((from_y, 4) if l else (from_x, 2))))
        pieces = own, from_c, from_x, from_y, send(from_x, 1), send(from_y, 1)
        where = (l, 0, 0, 0), (l, 0, 0, 1), (l, 1, 0, 0), (l, 0, 1, 0), (l, 1, 0, 1), (l, 0, 1, 1)
        outs[n] = place(outs[n], pieces, where, shapes[n])
        before = n
    corners[0], outs[before], *others = lax.optimization_barrier((corners[0], outs[before], *others))
    where = (0, 1, 1, 0), (1, 1, 1, 0), (0, 1, 1, 1), (1, 1, 1, 1)
    for n in range(len(outs)):
        pair = corners[2 * n : 2 * n + 2]
        if n:
            *pair, outs[n - 1] = lax.optimization_barrier((*pair, outs[n - 1]))
        pieces = *pair, *(send(t, 1) for t in pair)
        outs[n] = place(outs[n], pieces, where, shapes[n])
    return outs, others


def moments_of(m, v, g):
    return 0.9 * m + 0.1 * g, 0.95 * v + 0.05 * g * g


def weight_of(w, m, v):
    return (w - 0.02 * (m * lax.rsqrt(v + 1e-8) + 0.1 * w)).astype(BF)


def solution(mesh):
    def step(x, dy, wg, wu, wd, *moments):
        me = lax.axis_index("dp")
        x, dy = x[0], dy[0]

        gate, up, ht, at, h = forward(x, wg, wu, wd)
        *grads, factor = backward(at, dy, h, gate, up, ht, wg, wu, wd)
        factor = factor[0, 0]
        weights, m, v = (wg, wu, wd), moments[:3], moments[3:]
        owns, now = [], factor
        for n, w in enumerate(weights):
            rows = m[n].shape[1]
            for l in range(w.shape[0]):
                own = lax.dynamic_slice(w, (l, me * rows, 0), (1, rows, w.shape[2]))[0]
                own = weight_of(own.astype(F32), *moments_of(m[n][l], v[n][l], grads[n][l].astype(F32) * now))
                own, now = lax.optimization_barrier((own, now))
                owns.append(own)
        new = [moments_of(m[n], v[n], grads[n].astype(F32) * now) for n in range(3)]
        outs, others = gathered(owns, [w.shape for w in weights], [t for pair in zip(*new) for t in pair])
        return (*outs, *others)

    P = jax.sharding.PartitionSpec
    rows = P(None, "dp", None)
    return jax.shard_map(
        step,
        mesh=mesh,
        in_specs=(P(("rep", "dp")),) * 2 + (P(),) * 3 + (rows,) * 6,
        out_specs=(P("rep"),) * 3 + (P("rep", "dp", None),) * 6,
        check_vma=False,
    )
```

```python
import jax
import jax.numpy as jnp
from jax import lax
from jax.experimental import pallas as pl
from jax.experimental.pallas import tpu as pltpu


BF, F32 = jnp.bfloat16, jnp.float32
NB = 256
VM = 64 * 1024 * 1024 - 65536


def dot(a, b, ca=1, cb=0):
    return lax.dot_general(a, b, (((ca,), (cb,)), ((), ())), preferred_element_type=F32)


def normed(h):
    wide = h.astype(F32)
    scale = lax.rsqrt(jnp.mean(wide * wide, -1, keepdims=True) + 1e-6)
    return (wide * scale).astype(BF)


def params():
    return pltpu.CompilerParams(vmem_limit_bytes=VM, dimension_semantics=("arbitrary",))


def whole(shape):
    return pl.BlockSpec(shape, lambda j: (0,) * len(shape))


def cost(mm, by):
    return pl.CostEstimate(flops=mm, bytes_accessed=by, transcendentals=0)


def tiles(t, rt):
    return [pl.ds(i * rt, rt) for i in range(t // rt)]


def beside(ref, one, other):
    n = one.shape[1]
    ref[:, :n] = one[...]
    ref[:, n:] = other[...]


def forward(x, wg, wu, wd):
    t_, d = x.shape
    ff = wg.shape[2]
    n1, rt = ff // NB, 512
    n2 = t_ // rt

    def body(x_hbm, wg_ref, wu_ref, wd_hbm, gate_ref, up_ref, ht_ref, at_hbm, h_ref, xs, a, at, hid, w, wds, sem, wd_sem, at_sem):
        t = pl.program_id(0)
        second = t >= n1 + n2
        wd_load = pltpu.make_async_copy(wd_hbm.at[0], wds, wd_sem)
        early = pl.ds(0, t_ - 256)
        late = pl.ds(t_ - 256, 256)
        at_stores = [pltpu.make_async_copy(at, at_hbm.at[0], at_sem.at[0])]
        at_stores += [pltpu.make_async_copy(at.at[:, c], at_hbm.at[1, :, c], at_sem.at[i]) for i, c in enumerate((early, late))]

        @pl.when(t == 0)
        def _():
            loads = [pltpu.make_async_copy(x_hbm.at[r], xs.at[r], sem.at[i]) for i, r in enumerate(tiles(t_, rt))]
            for load in loads:
                load.start()
            wd_load.start()
            for i, load in enumerate(loads):
                load.wait()
                for r in range(i * rt, (i + 1) * rt, 256):
                    a[pl.ds(r, 256), :] = normed(xs[pl.ds(r, 256), :])

        @pl.when((t < n1) | second)
        def _():
            beside(w, wg_ref, wu_ref)
            j = jnp.where(second, t - n1 - n2, t)
            cols = pl.ds(pl.multiple_of(j * NB, NB), NB)
            part = pl.ds(pl.multiple_of(jnp.minimum(j, t_ // 256 - 1) * 256, 256), 256)
            at[:, part] = a[part, :].T
            for r in tiles(t_, rt):
                both = dot(a[r, :], w[...])
                gate, up = both[:, :NB], both[:, NB:]
                gate_ref[r, :] = gate
                up_ref[r, :] = up
                hidden = (jax.nn.silu(gate) * up).astype(BF)
                hid[r, cols] = hidden
                ht_ref[:, r] = hidden.T

        @pl.when(t == n1)
        def _():
            wd_load.wait()
            at_stores[0].start()

        @pl.when((t >= n1) & (t < n1 + n2))
        def _():
            r = pl.ds(pl.multiple_of((t - n1) * rt, rt), rt)
            h = xs[r, :] + dot(hid[r, :], wds[...]).astype(BF)
            h_ref[...] = h
            a[r, :] = normed(h)

        @pl.when(t == n1 + n2 - 1)
        def _():
            at_stores[0].wait()

        @pl.when(t == 2 * n1 + n2 - 2)
        def _():
            at_stores[1].start()

        @pl.when(t == 2 * n1 + n2 - 1)
        def _():
            at_stores[2].start()
            at_stores[1].wait()
            at_stores[2].wait()

    def layer(j):
        return jnp.where(j < n1 + n2, 0, 1)

    def block(j):
        return jnp.where(j < n1 + n2, jnp.minimum(j, n1 - 1), j - n1 - n2)

    anyw = pl.BlockSpec(memory_space=pl.ANY)
    wcol = pl.BlockSpec((None, d, NB), lambda j: (layer(j), 0, block(j)))
    gcol = pl.BlockSpec((None, t_, NB), lambda j: (layer(j), 0, block(j)))
    hrow = pl.BlockSpec((None, NB, t_), lambda j: (layer(j), block(j), 0))
    return pl.pallas_call(
        body,
        grid=(2 * n1 + n2,),
        in_specs=[anyw, wcol, wcol, anyw],
        out_specs=[gcol, gcol, hrow, anyw, pl.BlockSpec((rt, d), lambda j: (jnp.clip(j - n1, 0, n2 - 1), 0))],
        out_shape=[
            jax.ShapeDtypeStruct((2, t_, ff), F32),
            jax.ShapeDtypeStruct((2, t_, ff), F32),
            jax.ShapeDtypeStruct((2, ff, t_), BF),
            jax.ShapeDtypeStruct((2, d, t_), BF),
            jax.ShapeDtypeStruct((t_, d), BF),
        ],
        scratch_shapes=[
            pltpu.VMEM((t_, d), BF),
            pltpu.VMEM((t_, d), BF),
            pltpu.VMEM((d, t_), BF),
            pltpu.VMEM((t_, ff), BF),
            pltpu.VMEM((d, 2 * NB), BF),
            pltpu.VMEM((ff, d), BF),
            pltpu.SemaphoreType.DMA((n2,)),
            pltpu.SemaphoreType.DMA,
            pltpu.SemaphoreType.DMA((2,)),
        ],
        compiler_params=params(),
        cost_estimate=cost(10 * t_ * d * ff, 0),
        name="forward",
    )(x, wg, wu, wd)


def hidden_back(dh, gate, up):
    s = jax.nn.sigmoid(gate)
    sg = gate * s
    return (dh * up * (s + sg * (1 - s))).astype(BF), (dh * sg).astype(BF)


SLOTS = {True: (4, 5, 2, 6, 2, 4), False: (3, 3, 1, 3, 1, 2)}
MESH = pl.DeviceIdType.MESH
GU, DD = 256, 352


class Exchange:
    def __init__(self, rows, slots, squares, put, src, rc, sx, sy, rx, ry, s2, r2, sent, got):
        self.rows, self.slots = rows, slots
        self.src, self.rc, self.sx, self.sy, self.rx, self.ry, self.s2, self.r2 = src, rc, sx, sy, rx, ry, s2, r2
        self.sent, self.got, self.squares, self.put = sent, got, squares, put
        me = lax.axis_index("dp")
        self.me, self.others = me, [lax.rem(me + i, 8) for i in range(1, 8)]
        self.x, self.y, self.c = me // 4, me // 2 % 2, me % 2
        self.over_c, self.over_y, self.over_x = me + 1 - 2 * self.c, me + 2 - 4 * self.y, me + 4 - 8 * self.x

    def barrier(self):
        b = pltpu.get_barrier_semaphore()
        for other in self.others:
            pl.semaphore_signal(b, inc=1, device_id={"dp": other}, device_id_type=MESH)
        pl.semaphore_wait(b, len(self.others))

    def copy(self, n, slot, src, dst, other):
        return pltpu.make_async_remote_copy(
            src_ref=src, dst_ref=dst, send_sem=self.sent.at[n, slot], recv_sem=self.got.at[n, slot],
            device_id={"dp": other}, device_id_type=MESH,
        )

    def copies(self, stage, k):
        rows, h = self.rows, self.rows // 2
        SRC, RC, SX, RX, S2, R2 = self.slots
        if stage == 0:
            s, r = lax.rem(k, SRC), lax.rem(k, RC)
            return [self.copy(0, r, self.src.at[s, :, 1 - self.c, :rows], self.rc.at[r, :, :rows], self.over_c)]
        if stage == 1:
            s, r = lax.rem(k, SX), lax.rem(k, RX)
            return [
                self.copy(1, r, self.sx.at[s, :, :h], self.rx.at[r, :, :h], self.over_x),
                self.copy(2, r, self.sy.at[s, :, :h], self.ry.at[r, :, :h], self.over_y),
            ]
        s, r = lax.rem(k, S2), lax.rem(k, R2)
        return [
            self.copy(3, r, self.s2.at[s, 0, :h], self.r2.at[r, 0, :h], self.over_y),
            self.copy(4, r, self.s2.at[s, 1, :h], self.r2.at[r, 1, :h], self.over_x),
        ]

    def start(self, stage, k):
        for c in self.copies(stage, k):
            c.start()

    def chip(self, k, i, j, part):
        at = i * 2 + j
        return self.src[lax.rem(k, self.slots[0]), at, self.c, part, :].astype(F32) + self.rc[lax.rem(k, self.slots[1]), at, part, :].astype(F32)

    def stage(self, n, k):
        for c in self.copies(n - 1, k):
            c.wait()
        rows, h, x, y = self.rows, self.rows // 2, self.x, self.y
        a, b = slice(0, h), slice(h, rows)
        sx, rx, s2, r2 = (lax.rem(k, m) for m in self.slots[2:])
        if n == 1:
            for i in range(2):
                self.sx[sx, i, a, :] = self.chip(k, 1 - x, i, a).astype(BF)
                self.sy[sx, i, a, :] = self.chip(k, i, 1 - y, b).astype(BF)
        elif n == 2:
            self.s2[s2, 0, a, :] = (self.chip(k, x, 1 - y, a) + self.rx[rx, 1 - y, a, :].astype(F32)).astype(BF)
            self.s2[s2, 1, a, :] = (self.chip(k, 1 - x, y, b) + self.ry[rx, 1 - x, a, :].astype(F32)).astype(BF)
        else:
            first = self.chip(k, x, y, a) + self.rx[rx, y, a, :].astype(F32) + self.r2[r2, 0, a, :].astype(F32)
            second = self.chip(k, x, y, b) + self.ry[rx, x, a, :].astype(F32) + self.r2[r2, 1, a, :].astype(F32)
            first, second = first.astype(BF), second.astype(BF)
            self.put(k, first, second)
            for g in (first, second):
                g = g.astype(F32)
                self.squares[...] += jnp.sum(g * g, 0, keepdims=True)
        if n < 3:
            self.start(n, k)

    def due(self, n, k, when):
        @pl.when(when)
        def _():
            if n:
                self.stage(n, k)
            else:
                self.start(0, k)


def exchange_scratch(rows, slots):
    half = (2, rows // 2, NB)
    SRC, RC, SX, RX, S2, R2 = slots
    shapes = [(SRC, 4, 2, rows, NB), (RC, 4, rows, NB), (SX, *half), (SX, *half), (RX, *half), (RX, *half), (S2, *half), (R2, *half)]
    return [pltpu.VMEM(shape, BF) for shape in shapes] + [pltpu.SemaphoreType.DMA((5, max(slots)))] * 2


def backward(at, dy, h, gate, up, ht, wg, wu, wd):
    _, d, t_ = at.shape
    ff = wg.shape[2]
    n, n_dd = ff // NB, d // NB
    last = 2 * n + 3
    count = wg.size + wu.size + wd.size
    skip = (n + 1) // 2 - n_dd

    def body(
        at_hbm, dy_hbm, h_hbm, g_hbm, u_hbm, ht_hbm, wg_ref, wu_ref, wd_ref, rg_ref, ru_ref, rd_ref, factor_ref,
        dh, hs, acc, w, at, gu, hbuf, dgu, sq, sums, sums_got, sums_sem, at_sem, dh_sem, h_sem, gu_sem, ht_sem, *refs,
    ):
        src, src_d = refs[0], refs[10]
        t = pl.program_id(0)
        inner = t < n

        def put_gu(k, first, second):
            rg_ref[...] = first
            ru_ref[...] = second

        def put_d(k, first, second):
            rd_ref[: DD // 2, :] = first
            rd_ref[DD // 2 :, :] = second

        ex = Exchange(GU, SLOTS[True], sq, put_gu, *refs[:10])
        ex_d = Exchange(DD, SLOTS[False], sq, put_d, *refs[10:])
        at_loads = [pltpu.make_async_copy(at_hbm.at[layer], at, at_sem) for layer in range(2)]
        dh_load = pltpu.make_async_copy(dy_hbm, dh, dh_sem)
        h_load = pltpu.make_async_copy(h_hbm, hs, h_sem)

        def gu_loads(j):
            cols = pl.ds(pl.multiple_of(lax.rem(j, n) * NB, NB), NB)
            return [pltpu.make_async_copy(r.at[1 - j // n, :, cols], gu.at[i], gu_sem.at[i]) for i, r in enumerate((g_hbm, u_hbm))]

        def ht_load():
            rows = pl.ds(pl.multiple_of(lax.rem(t, 2) * 4 * DD, 4 * DD), 4 * DD)
            return pltpu.make_async_copy(ht_hbm.at[1 - t // n, rows], hbuf, ht_sem)

        @pl.when(t == 0)
        def _():
            dh_load.start()
            for load in gu_loads(0):
                load.start()
            at_loads[1].start()
            sq[...] = jnp.zeros_like(sq)
            for r in tiles(t_, 256):
                acc[r, :] = jnp.zeros((256, d), F32)
            ex.barrier()
            dh_load.wait()

        pair, even = t // 2, lax.rem(t, 2) == 0
        odd = lax.rem(t, 2) == 1
        start = 2 * (n_dd + skip)
        making_d = (t < 2 * n_dd) | ((t >= start) & (t < start + 2 * n_dd))
        column = jnp.where(t < start, pair, pair - n_dd - skip)

        @pl.when(making_d)
        def _():
            ht_load().start()

        def due_d(stage, later, when):
            k = pair - later
            ex_d.due(stage, k, when & (k >= 0) & (k < n_dd))
            ex_d.due(stage, k - skip, when & (k >= n_dd + skip) & (k < 2 * n_dd + skip))

        ex.due(0, t - 1, (t >= 1) & (t <= 2 * n))
        due_d(0, 1, even)
        ex.due(2, t - 3, (t >= 3) & (t <= 2 * n + 2))
        due_d(2, 2, even)

        @pl.when(t == n)
        def _():
            at_loads[0].start()
            h_load.wait()
            for r in tiles(t_, 256):
                da = acc[r, :].astype(BF).astype(F32)
                wide = hs[r, :].astype(F32)
                scale = lax.rsqrt(jnp.mean(wide * wide, -1, keepdims=True) + 1e-6)
                along = jnp.sum(da * wide, -1, keepdims=True) * (scale * scale * scale / d)
                dh[r, :] = dh[r, :] + (da * scale - wide * along).astype(BF)

        def hidden_units(inner):
            for load in gu_loads(t):
                load.wait()
            if inner:
                beside(w, wg_ref, wu_ref)
            for r in tiles(t_, 512):
                dp = dot(dh[r, :], wd_ref[...], 1, 1).astype(BF).astype(F32)
                dgt, dut = hidden_back(dp, gu[0, r, :], gu[1, r, :])
                dgu[r, :NB] = dgt
                dgu[r, NB:] = dut
                if inner:
                    acc[r, :] += dot(jnp.concatenate([dgt, dut], 1), w[...], 1, 1)

        @pl.when(inner)
        def _():
            hidden_units(True)

        @pl.when((t >= n) & (t < 2 * n))
        def _():
            hidden_units(False)

        @pl.when(t < 2 * n - 1)
        def _():
            for load in gu_loads(t + 1):
                load.start()

        ex.due(1, t - 1, (t >= 1) & (t <= 2 * n))
        due_d(1, 1, even)
        ex.due(3, t - 4, (t >= 4) & (t <= 2 * n + 3))
        due_d(3, 2, odd)

        @pl.when(t == 0)
        def _():
            h_load.start()
            at_loads[1].wait()

        @pl.when(t == n)
        def _():
            at_loads[0].wait()

        @pl.when(t < 2 * n)
        def _():
            slot = lax.rem(t, SLOTS[True][0])
            for i in range(2):
                both = dot(at[pl.ds(i * d // 2, d // 2), :], dgu[...]).astype(BF)
                src[slot, 2 * i : 2 * i + 2, :, : GU // 2, :] = both[:, :NB].reshape(2, 2, GU // 2, NB)
                src[slot, 2 * i : 2 * i + 2, :, GU // 2 :, :] = both[:, NB:].reshape(2, 2, GU // 2, NB)

        @pl.when(making_d)
        def _():
            ht_load().wait()
            slot = lax.rem(jnp.where(t < start, pair, pair - skip), SLOTS[False][0])
            cols = pl.ds(pl.multiple_of(column * NB, NB), NB)
            for i in range(2):
                rows = pl.ds(i * 2 * DD, 2 * DD)
                src_d[slot, 2 * lax.rem(t, 2) + i] = dot(hbuf[rows, :], dh[:, cols]).astype(BF).reshape(2, DD, NB)

        @pl.when(t == last)
        def _():
            own = jnp.broadcast_to(jnp.sum(sq[...], 1, keepdims=True), (8, 128))
            sums[...] = own
            sums_got[ex.me] = own
            copies = [
                pltpu.make_async_remote_copy(
                    src_ref=sums, dst_ref=sums_got.at[ex.me], send_sem=sums_sem.at[0, i], recv_sem=sums_sem.at[1, i],
                    device_id={"dp": other}, device_id_type=MESH,
                )
                for i, other in enumerate(ex.others)
            ]
            for copy in copies:
                copy.start()
            for copy in copies:
                copy.wait()
            total = sums_got[0]
            for i in range(1, 8):
                total = total + sums_got[i]
            factor = jnp.minimum(1.0, 0.5 * lax.rsqrt(total / count + 1e-30))
            factor_ref[...] = factor[:1, :1]

    def tick(j):
        return jnp.minimum(j, 2 * n - 1)

    def gu_out(j):
        k = jnp.clip(j - 4, 0, 2 * n - 1)
        return (1 - k // n, 0, k % n)

    def d_out(j):
        k = jnp.maximum(j - 5, 0) // 2
        k = jnp.where(k < n_dd + skip, jnp.minimum(k, n_dd - 1), jnp.minimum(k - skip, 2 * n_dd - 1))
        return (1 - k // n_dd, 0, k % n_dd)

    anyw = pl.BlockSpec(memory_space=pl.ANY)
    wcol = pl.BlockSpec((None, d, NB), lambda j: (1, 0, jnp.minimum(j, n - 1)))
    wrow = pl.BlockSpec((None, NB, d), lambda j: (1 - tick(j) // n, tick(j) % n, 0))
    out_gu = pl.BlockSpec((None, d // 8, NB), gu_out)
    return pl.pallas_call(
        body,
        grid=(last + 1,),
        in_specs=[anyw] * 6 + [wcol, wcol, wrow],
        out_specs=[out_gu, out_gu, pl.BlockSpec((None, ff // 8, NB), d_out), whole((1, 1))],
        out_shape=[
            jax.ShapeDtypeStruct((2, d // 8, ff), BF),
            jax.ShapeDtypeStruct((2, d // 8, ff), BF),
            jax.ShapeDtypeStruct((2, ff // 8, d), BF),
            jax.ShapeDtypeStruct((1, 1), F32),
        ],
        scratch_shapes=[
            pltpu.VMEM((t_, d), BF),
            pltpu.VMEM((t_, d), BF),
            pltpu.VMEM((t_, d), F32),
            pltpu.VMEM((d, 2 * NB), BF),
            pltpu.VMEM((d, t_), BF),
            pltpu.VMEM((2, t_, NB), F32),
            pltpu.VMEM((4 * DD, t_), BF),
            pltpu.VMEM((t_, 2 * NB), BF),
            pltpu.VMEM((1, NB), F32),
            pltpu.VMEM((8, 128), F32),
            pltpu.VMEM((8, 8, 128), F32),
            pltpu.SemaphoreType.DMA((2, 7)),
            pltpu.SemaphoreType.DMA,
            pltpu.SemaphoreType.DMA,
            pltpu.SemaphoreType.DMA,
            pltpu.SemaphoreType.DMA((2,)),
            pltpu.SemaphoreType.DMA,
        ]
        + exchange_scratch(GU, SLOTS[True])
        + exchange_scratch(DD, SLOTS[False]),
        compiler_params=pltpu.CompilerParams(
            vmem_limit_bytes=VM, dimension_semantics=("arbitrary",), collective_id=1, has_side_effects=True
        ),
        cost_estimate=cost(20 * t_ * d * ff, 0),
        name="backward",
    )(at, dy, h, gate, up, ht, wg, wu, wd)


def swap(bit):
    return [(i, i ^ bit) for i in range(8)]


def send(t, bit):
    return lax.ppermute(t, "dp", swap(bit))


def place(out, pieces, where, shape):
    rows, n = pieces[0].shape
    count = len(pieces)

    def body(*refs):
        pieces, (o_ref, held, sems) = refs[:count], refs[-3:]
        me = lax.axis_index("dp")
        x, y, c = me // 4, me // 2 % 2, me % 2
        loads = [pltpu.make_async_copy(p, held.at[i], sems.at[0, i]) for i, p in enumerate(pieces)]
        stores = []
        for load in loads:
            load.start()
        for i, (load, (layer, fx, fy, fc)) in enumerate(zip(loads, where)):
            block = (abs(fx - x) * 2 + abs(fy - y)) * 2 + abs(fc - c)
            at = pl.ds(pl.multiple_of(block * rows, rows), rows)
            load.wait()
            stores.append(pltpu.make_async_copy(held.at[i], o_ref.at[layer, at], sems.at[1, i]))
            stores[-1].start()
        for store in stores:
            store.wait()

    args = (*pieces, *(() if out is None else (out,)))
    return pl.pallas_call(
        body,
        in_specs=[pl.BlockSpec(memory_space=pl.ANY)] * len(args),
        out_specs=pl.BlockSpec(memory_space=pl.ANY),
        out_shape=jax.ShapeDtypeStruct(shape, BF),
        scratch_shapes=[pltpu.VMEM((count, rows, n), BF), pltpu.SemaphoreType.DMA((2, count))],
        input_output_aliases={} if out is None else {count: 0},
        compiler_params=pltpu.CompilerParams(vmem_limit_bytes=VM),
        cost_estimate=cost(2_000_000_000 * count, 4 * count * rows * n),
        name="place",
    )(*args)


def gathered(owns, shapes, others):
    first = [(own, send(own, 4), send(own, 2), send(own, 1)) for own in owns]
    outs, corners, before = [None] * len(shapes), [], None
    for i, (own, from_x, from_y, from_c) in enumerate(first):
        n, l = divmod(i, 2)
        if i:
            from_x, from_y, outs[before] = lax.optimization_barrier((from_x, from_y, outs[before]))
        corners.append(send(*((from_y, 4) if l else (from_x, 2))))
        pieces = own, from_c, from_x, from_y, send(from_x, 1), send(from_y, 1)
        where = (l, 0, 0, 0), (l, 0, 0, 1), (l, 1, 0, 0), (l, 0, 1, 0), (l, 1, 0, 1), (l, 0, 1, 1)
        outs[n] = place(outs[n], pieces, where, shapes[n])
        before = n
    corners[0], outs[before], *others = lax.optimization_barrier((corners[0], outs[before], *others))
    where = (0, 1, 1, 0), (1, 1, 1, 0), (0, 1, 1, 1), (1, 1, 1, 1)
    for n in range(len(outs)):
        pair = corners[2 * n : 2 * n + 2]
        if n:
            *pair, outs[n - 1] = lax.optimization_barrier((*pair, outs[n - 1]))
        swapped = [send(t, 1) for t in pair]
        outs[n] = place(outs[n], pair, where[:2], shapes[n])
        outs[n] = place(outs[n], swapped, where[2:], shapes[n])
    return outs, others


def moments_of(m, v, g):
    return 0.9 * m + 0.1 * g, 0.95 * v + 0.05 * g * g


def weight_of(w, m, v):
    return (w - 0.02 * (m * lax.rsqrt(v + 1e-8) + 0.1 * w)).astype(BF)


def solution(mesh):
    def step(x, dy, wg, wu, wd, *moments):
        me = lax.axis_index("dp")
        x, dy = x[0], dy[0]

        gate, up, ht, at, h = forward(x, wg, wu, wd)
        *grads, factor = backward(at, dy, h, gate, up, ht, wg, wu, wd)
        factor = factor[0, 0]
        weights, m, v = (wg, wu, wd), moments[:3], moments[3:]
        owns, now = [], factor
        for n, w in enumerate(weights):
            rows = m[n].shape[1]
            for l in range(w.shape[0]):
                own = lax.dynamic_slice(w, (l, me * rows, 0), (1, rows, w.shape[2]))[0]
                own = weight_of(own.astype(F32), *moments_of(m[n][l], v[n][l], grads[n][l].astype(F32) * now))
                own, now = lax.optimization_barrier((own, now))
                owns.append(own)
        new = [moments_of(m[n], v[n], grads[n].astype(F32) * now) for n in range(3)]
        outs, others = gathered(owns, [w.shape for w in weights], [t for pair in zip(*new) for t in pair])
        return (*outs, *others)

    P = jax.sharding.PartitionSpec
    rows = P(None, "dp", None)
    return jax.shard_map(
        step,
        mesh=mesh,
        in_specs=(P(("rep", "dp")),) * 2 + (P(),) * 3 + (rows,) * 6,
        out_specs=(P("rep"),) * 3 + (P("rep", "dp", None),) * 6,
        check_vma=False,
    )
```
